512 devices in a mesh: node: 128 (over z, x, core), chan: 4 (over y).
Axes of the slice: x: 4, y: 4, z: 16, core: 2. Of those that a mesh axis runs over, the one named last changes fastest.
Arguments:
- nodes: bfloat16 [16384, 512], P('node'), may hold values from -6 to 6
- edges: bfloat16 [49152, 512], P('node'), may hold values from -6 to 6
- grad_nodes_in: bfloat16 [16384, 512], P('node'), may hold values from -6 to 6
- grad_edges_in: bfloat16 [49152, 512], P('node'), may hold values from -6 to 6
- edge_in_weight: bfloat16 [1536, 512], P(None, 'chan'), may hold values from -0.15625 to 0.15625
- edge_bias: float32 [512], P('chan'), may hold values from -4 to 4
- edge_out_weight: bfloat16 [512, 512], P('chan'), may hold values from -0.25 to 0.25
- node_in_weight: bfloat16 [1024, 512], P(None, 'chan'), may hold values from -0.1875 to 0.1875
- node_bias: float32 [512], P('chan'), may hold values from -4 to 4
- node_out_weight: bfloat16 [512, 512], P('chan'), may hold values from -0.25 to 0.25
- senders: int32 [49152], P('node'), may hold values from 0 to 255
- receivers: int32 [49152], P('node'), may hold values from 0 to 127, as said below
- valid_counts: int32 [384], P('node'), may hold values from 1 to 128
- send_list: int32 [16384, 1], P('node'), may hold values from 0 to 127
Outputs:
- grad_nodes: bfloat16 [16384, 512], P('node', 'chan')
- grad_edges: bfloat16 [49152, 512], P('node', 'chan')
- grad_edge_in: float32 [1536, 512], P('node', 'chan')
- grad_edge_out: float32 [512, 512], P('chan', 'node')
- grad_node_in: float32 [1024, 512], P('node', 'chan')
- grad_node_out: float32 [512, 512], P('chan', 'node')
The draws below stay inside these ranges and needn't reach their ends.
Inputs may be any that keep to these rules, and one draw needn't show every extreme that they name: `senders`: below 128: a node of the slot's own owner; otherwise 128 + p + j, the j-th node that owner p sends to the slot's owner. `receivers`: A node number on the slot's owner, nondecreasing within each owner's 384 slots. `valid_counts`: the live slots of a block are its first ones. `send_list`: row p * 128 + q holds node numbers of owner p that owner q reads.
All inputs are finite; a program needn't handle non-finite values.
Results may differ from the reference program's by a relative error of at most 0.011.
Values may be sent and summed in bfloat16 or wider, within the bound.
A program may use at most 64 MiB of HBM per device.

```python
import jax
import jax.numpy as jnp
from jax import lax

D = 512
H = 512
N_DEV = 128
E_DEV = 384
BLOCK = 128
SLOT = 1
OWNERS = 128
HALO = 128
NODES = 16384
EDGES = 49152


def draw_receivers(key, part):
    values = jax.random.randint(key, (OWNERS, E_DEV), 0, N_DEV)
    return jnp.sort(values, axis=1).reshape(-1).astype(jnp.int32)


def plant(drawn, rng, least, high):
    extent = drawn.shape
    spot = [jax.random.randint(jax.random.fold_in(rng, axis), (), 0, extent[axis]) for axis in range(len(extent))]
    drawn = drawn.at[tuple(spot)].set(least)
    longest = extent.index(max(extent))
    spot[longest] = (spot[longest] + 1) % extent[longest]
    return drawn.at[tuple(spot)].set(high)


def level_of(key, shape, cuts, least, high):
    factor_of = 1.0
    for dim, blocks in cuts:
        heights = jax.random.uniform(jax.random.fold_in(jax.random.fold_in(key, 6), dim), (blocks,), jnp.float32, least / len(cuts), high / len(cuts))
        factor_of = factor_of * jnp.repeat(jnp.exp(heights), shape[dim] // blocks).reshape((-1,) + (1,) * (len(shape) - 1 - dim))
    return factor_of


def noise(stream_key, extent, deviation, limit, shards=(), kind=jnp.bfloat16):
    values = deviation * jax.random.normal(stream_key, extent, jnp.float32)
    if shards:
        values = values * level_of(stream_key, extent, shards, -0.22, 0.18)
    return jnp.clip(values, -limit, limit).astype(kind)


def setup_inputs(seed: int = 0) -> dict:
    seeds = jax.random.split(jax.random.key(seed), 15)
    nodes = noise(seeds[0], (NODES, D), 1.0, 6.0, ((0, 128),))
    edges = noise(seeds[1], (EDGES, D), 1.0, 6.0, ((0, 128),))
    grad_nodes_in = noise(seeds[2], (NODES, D), 1.0, 6.0, ((0, 128),))
    grad_edges_in = noise(seeds[3], (EDGES, D), 1.0, 6.0, ((0, 128),))
    edge_in_weight = noise(seeds[4], (3 * D, H), (3 * D) ** -0.5, 0.15625, ((1, 4),))
    edge_bias = noise(seeds[5], (H,), 1.0, 4.0, ((0, 4),), jnp.float32)
    edge_out_weight = noise(seeds[6], (H, D), H ** -0.5, 0.25, ((0, 4),))
    node_in_weight = noise(seeds[7], (2 * D, H), (2 * D) ** -0.5, 0.1875, ((1, 4),))
    node_bias = noise(seeds[8], (H,), 1.0, 4.0, ((0, 4),), jnp.float32)
    node_out_weight = noise(seeds[9], (H, D), H ** -0.5, 0.25, ((0, 4),))
    senders = plant(jax.random.randint(seeds[10], (EDGES,), 0, N_DEV + HALO), jax.random.fold_in(seeds[10], 1), 0, (N_DEV + HALO) - 1).astype(jnp.int32)
    receivers = draw_receivers(jax.random.fold_in(seeds[14], 71), 0)
    valid_counts = plant(jax.random.randint(seeds[12], (EDGES // BLOCK,), 1, BLOCK + 1), jax.random.fold_in(seeds[12], 1), 1, BLOCK).astype(jnp.int32)
    send_list = plant(jax.random.randint(seeds[13], (OWNERS * OWNERS, SLOT), 0, N_DEV), jax.random.fold_in(seeds[13], 1), 0, N_DEV - 1).astype(jnp.int32)
    return dict(nodes=nodes, edges=edges, grad_nodes_in=grad_nodes_in, grad_edges_in=grad_edges_in, edge_in_weight=edge_in_weight, edge_bias=edge_bias, edge_out_weight=edge_out_weight, node_in_weight=node_in_weight, node_bias=node_bias, node_out_weight=node_out_weight, senders=senders, receivers=receivers, valid_counts=valid_counts, send_list=send_list)


def silu_parts(preact):
    logistic = jax.nn.sigmoid(preact)
    return preact * logistic, logistic * (1.0 + preact * (1.0 - logistic))


def contract(left_mat, right_mat, left_dim, right_dim):
    return lax.dot_general(left_mat, right_mat, (((left_dim,), (right_dim,)), ((), ())), preferred_element_type=jnp.float32)


def reference(nodes, edges, grad_nodes_in, grad_edges_in, edge_in_weight, edge_bias, edge_out_weight, node_in_weight, node_bias, node_out_weight, senders, receivers, valid_counts, send_list):
    owner_ids = jnp.arange(EDGES, dtype=jnp.int32) // E_DEV
    offset = jnp.maximum(senders - N_DEV, 0).astype(jnp.int32)
    peer_ids = offset // SLOT
    slot_ids = offset % SLOT
    remote = (send_list[peer_ids * OWNERS + owner_ids, slot_ids] + peer_ids * N_DEV).astype(jnp.int32)
    sender_rows = jnp.where(senders < N_DEV, owner_ids * N_DEV + senders, remote).astype(jnp.int32)
    receiver_rows = (owner_ids * N_DEV + receivers).astype(jnp.int32)
    position = jnp.arange(EDGES, dtype=jnp.int32) % BLOCK
    live_mask = (position < jnp.repeat(valid_counts, BLOCK)).astype(jnp.float32)[:, None]
    stacked = jnp.concatenate([edges, nodes[sender_rows], nodes[receiver_rows]], axis=1)
    edge_pre = jnp.dot(stacked, edge_in_weight, preferred_element_type=jnp.float32) + edge_bias
    edge_act, edge_slope = silu_parts(edge_pre)
    hidden = (edge_act * live_mask).astype(jnp.bfloat16)
    hidden_sums = jax.ops.segment_sum(hidden.astype(jnp.float32), receiver_rows, num_segments=NODES).astype(jnp.bfloat16)
    aggregate = jnp.dot(hidden_sums, edge_out_weight, preferred_element_type=jnp.float32).astype(jnp.bfloat16)
    node_cat = jnp.concatenate([nodes, aggregate], axis=1)
    node_pre = jnp.dot(node_cat, node_in_weight, preferred_element_type=jnp.float32) + node_bias
    node_act, node_slope = silu_parts(node_pre)
    node_hidden = node_act.astype(jnp.bfloat16)
    node_pre_grad = (contract(grad_nodes_in, node_out_weight, 1, 1) * node_slope).astype(jnp.bfloat16)
    grad_node_out = contract(node_hidden, grad_nodes_in, 0, 0)
    grad_node_in = contract(node_cat, node_pre_grad, 0, 0)
    node_back = contract(node_pre_grad, node_in_weight, 1, 1)
    grad_aggregate = node_back[:, D:]
    message_grad = (grad_edges_in.astype(jnp.float32) + grad_aggregate[receiver_rows]).astype(jnp.bfloat16)
    edge_pre_grad = (contract(message_grad, edge_out_weight, 1, 1) * edge_slope * live_mask).astype(jnp.bfloat16)
    grad_edge_out = contract(hidden, message_grad, 0, 0)
    grad_edge_in = contract(stacked, edge_pre_grad, 0, 0)
    edge_back = contract(edge_pre_grad, edge_in_weight, 1, 1)
    grad_edges = (grad_edges_in.astype(jnp.float32) + edge_back[:, :D]).astype(jnp.bfloat16)
    node_terms = jax.ops.segment_sum(edge_back[:, D:2 * D], sender_rows, num_segments=NODES)
    node_terms = node_terms + jax.ops.segment_sum(edge_back[:, 2 * D:], receiver_rows, num_segments=NODES)
    grad_nodes = (grad_nodes_in.astype(jnp.float32) + node_back[:, :D] + node_terms).astype(jnp.bfloat16)
    return grad_nodes, grad_edges, grad_edge_in, grad_edge_out, grad_node_in, grad_node_out
```

```python
import functools

import jax
import jax.numpy as jnp
from jax import lax
from jax.experimental import pallas as pl
from jax.experimental.pallas import tpu as pltpu
from jax.sharding import Mesh
from jax.sharding import PartitionSpec as P

NODE = ("z", "x", "c")
MESH = pl.DeviceIdType.MESH
F32 = jnp.float32
BF16 = jnp.bfloat16


def dot(a, b):
    return jnp.dot(a, b, preferred_element_type=F32)


def dot_t(a, b):
    return lax.dot_general(a, b, (((1,), (1,)), ((), ())), preferred_element_type=F32)


def t_dot(a, b):
    return lax.dot_general(a, b, (((0,), (0,)), ((), ())), preferred_element_type=F32)


def iota(shape, dim):
    return lax.broadcasted_iota(jnp.int32, shape, dim)


def hot(cond):
    return jnp.where(cond, 1.0, 0.0).astype(BF16)


def two_parts(v):
    high = v.astype(BF16)
    return high, (v - high.astype(F32)).astype(BF16)


def sigmoid(v):
    return 1.0 / (1.0 + jnp.exp(-v))


def kernel(
    nz,
    nx,
    ny,
    sl_ref,
    snd_ref,
    rcv_ref,
    vc_ref,
    n_ref,
    e_ref,
    gn_ref,
    ge_ref,
    win_ref,
    be_ref,
    wout_ref,
    wn_ref,
    bn_ref,
    wno_ref,
    o_nodes,
    o_edges,
    o_ei,
    o_eo,
    o_ni,
    o_no,
    out1,
    r1,
    out2,
    r2,
    wout_g,
    wn2_g,
    rows_g,
    wn1_g,
    hs_b,
    hs_g,
    npg_b,
    npg_g,
    epg_b,
    epg_g,
    ga_f,
    gb_f,
    g1,
    g2,
    g3,
    g4,
    ha,
    hb,
    ca,
    cb,
    xa,
    xb,
    rxa,
    rxb,
    za,
    zb,
    rza,
    rzb,
    s_out,
    s_a,
    s_mid,
    s_b,
    send,
    recv,
):
    z, x, c, y = (lax.axis_index(a) for a in ("z", "x", "c", "y"))
    nxc = 2 * nx
    owners = nz * nxc
    nd, d_feat = n_ref.shape
    ed = e_ref.shape[0]
    hs_w = wout_ref.shape[0]
    fs_w = d_feat // ny
    block = ed // vc_ref.shape[0]

    def by(**kw):
        return kw

    z_off = lambda d: by(z=lax.rem(z + d, nz))
    y_off = lambda d: by(y=lax.rem(y + d, ny))
    xc_off = lambda k: by(x=lax.rem(x + k // 2, nx), c=c if k % 2 == 0 else 1 - c)
    xc_back = lambda k: by(x=lax.rem(x + nx - k // 2, nx), c=c if k % 2 == 0 else 1 - c)
    z_back = lambda d: by(z=lax.rem(z + nz - d, nz))

    barrier = pltpu.get_barrier_semaphore()
    peers = (
        [z_off(d) for d in range(1, nz)]
        + [xc_off(k) for k in range(1, nxc)]
        + [y_off(d) for d in range(1, ny)]
    )
    for peer in peers:
        pl.semaphore_signal(barrier, inc=1, device_id=peer, device_id_type=MESH)

    def push(phase, src, dst, peer):
        pltpu.make_async_remote_copy(
            src_ref=src,
            dst_ref=dst,
            send_sem=send.at[phase],
            recv_sem=recv.at[phase],
            device_id=peer,
            device_id_type=MESH,
        ).start()

    def arrived(phase, ref):
        pltpu.make_async_copy(ref, ref, recv.at[phase]).wait()

    def left(phase, ref):
        pltpu.make_async_copy(ref, ref, send.at[phase]).wait()

    nodes = n_ref[...]
    r_q = iota((owners, owners), 1)
    k_of, dz_of = r_q // nz, r_q % nz
    q_of = (
        ((z + dz_of) & (nz - 1)) * nxc
        + ((x + (k_of >> 1)) & (nx - 1)) * 2
        + (c ^ (k_of & 1))
    )
    perm_q = hot(iota((owners, owners), 0) == q_of)
    sl_hot = hot(iota((nd, owners), 0) == sl_ref[...])
    sl_perm = dot(sl_hot, perm_q).astype(BF16)
    rows_out = t_dot(sl_perm, nodes).astype(BF16)
    for k in range(nxc):
        out1[k] = rows_out[k * nz : (k + 1) * nz]
    r1[0] = rows_out[0:nz]

    pl.semaphore_wait(barrier, len(peers))

    for k in range(1, nxc):
        push(0, out1.at[k], r1.at[k], xc_off(k))
    for d in range(1, ny):
        push(2, wout_ref, wout_g.at[d - 1], y_off(d))
    for d in range(1, ny):
        push(3, wn_ref.at[1], wn2_g.at[d - 1], y_off(d))

    t_i = iota((owners, owners), 0)
    stage = hot(iota((owners, owners), 1) == (t_i % nxc) * nz + t_i // nxc)
    arrived(0, r1.at[pl.ds(1, nxc - 1)])
    second = dot(stage, r1[...].reshape(owners, d_feat)).astype(BF16)
    for d in range(nz):
        out2[d] = second[d * nxc : (d + 1) * nxc]
    r2[0] = second[0:nxc]
    for d in range(nz - 1, 0, -1):
        push(1, out2.at[d], r2.at[d], z_off(d))

    snd, rcv = snd_ref[...], rcv_ref[...]
    t_e = iota((owners, ed), 0)
    k_t, dz_t = t_e % nxc, t_e // nxc
    p_t = (
        ((z - dz_t) & (nz - 1)) * nxc
        + ((x - (k_t >> 1)) & (nx - 1)) * 2
        + (c ^ (k_t & 1))
    )
    hot_st = hot(iota((nd, ed), 0) == snd)
    hot_ht = hot(p_t + nd == snd)
    hot_rt = hot(iota((nd, ed), 0) == rcv)

    def picked(onehot_t, table):
        high, low = two_parts(table)
        return t_dot(onehot_t, high) + t_dot(onehot_t, low)

    live = jnp.concatenate(
        [
            jnp.where(iota((block, hs_w), 0) < vc_ref[b], 1.0, 0.0)
            for b in range(ed // block)
        ],
        axis=0,
    )
    edges = e_ref[...]
    base = (
        dot(edges, win_ref[0])
        + be_ref[...]
        + picked(hot_st, dot(nodes, win_ref[1]))
        + picked(hot_rt, dot(nodes, win_ref[2]))
    )
    ge = ge_ref[...]
    wout = wout_ref[...]
    ge_w = dot_t(ge, wout)
    gn = gn_ref[...]
    gn_w = dot_t(gn, wno_ref[...])
    base_n = dot(nodes, wn_ref[0]) + bn_ref[...]

    arrived(1, r2.at[pl.ds(1, nz - 1)])
    halo = r2[...].reshape(owners, d_feat)
    pre = base + picked(hot_ht, dot(halo, win_ref[1]))
    sg = sigmoid(pre)
    hidden = (pre * sg * live).astype(BF16)
    slope = sg * (1.0 + pre * (1.0 - sg)) * live
    hs = dot(hot_rt, hidden).astype(BF16)
    hs_b[...] = hs
    for d in range(1, ny):
        push(4, hs_b, hs_g.at[d - 1], y_off(d))
    geo = t_dot(ge, hidden)
    arrived(2, wout_g)
    arrived(4, hs_g)
    agg = dot(hs, wout)
    for d in range(1, ny):
        agg += dot(hs_g[d - 1], wout_g[d - 1])
    agg = agg.astype(BF16)

    npre = base_n + dot(agg, wn_ref[1])
    nsg = sigmoid(npre)
    nhid = (npre * nsg).astype(BF16)
    npg = (gn_w * (nsg * (1.0 + npre * (1.0 - nsg)))).astype(BF16)
    npg_b[...] = npg
    for d in range(1, ny):
        push(5, npg_b, npg_g.at[d - 1], y_off(d))
    for d in range(1, ny):
        yd = pl.multiple_of(lax.rem(y + d, ny) * fs_w, fs_w)
        push(6, win_ref.at[:, pl.ds(yd, fs_w)], rows_g.at[d - 1], y_off(d))
        push(7, wn_ref.at[0, pl.ds(yd, fs_w)], wn1_g.at[d - 1], y_off(d))
    g4[...] = t_dot(gn, nhid)
    g2[0:d_feat] = t_dot(nodes, npg)
    g2[d_feat:] = t_dot(agg, npg)
    arrived(3, wn2_g)
    arrived(5, npg_g)
    grad_agg = dot_t(npg, wn_ref[1])
    for d in range(1, ny):
        grad_agg += dot_t(npg_g[d - 1], wn2_g[d - 1])
    grad_agg = grad_agg.astype(BF16)
    epg = ((ge_w + picked(hot_rt, dot_t(grad_agg, wout))) * slope).astype(BF16)
    epg_b[...] = epg
    for d in range(1, ny):
        push(8, epg_b, epg_g.at[d - 1], y_off(d))
    g3[...] = geo + t_dot(grad_agg, hs)

    ni, eo, ei = 2 * d_feat // owners, d_feat // owners, 3 * d_feat // owners
    eip = gb_f.shape[3]

    def owner(n):
        return n % 2, (n // 2) % nx, n // nxc

    for n in range(owners):
        oc, ox, oz = owner(n)
        at = ga_f.at[oc, ox, oz]
        at[0:ni] = g2[n * ni : (n + 1) * ni]
        at[ni : ni + eo] = g3[n * eo : (n + 1) * eo]
        at[ni + eo : ni + 2 * eo] = g4[n * eo : (n + 1) * eo]
    ha[...] = ga_f[...].astype(BF16)
    push(9, ha.at[1 - c], ca, by(c=1 - c))

    s_hot = dot(hot_st, epg).astype(BF16)
    h_hot = dot(hot_ht, epg).astype(BF16)
    r_hot = dot(hot_rt, epg).astype(BF16)
    g1[0:d_feat] = t_dot(edges, epg)
    g1[d_feat : 2 * d_feat] = t_dot(nodes, s_hot) + t_dot(halo, h_hot)
    g1[2 * d_feat :] = t_dot(nodes, r_hot)
    for n in range(owners):
        oc, ox, oz = owner(n)
        at = gb_f.at[oc, ox, oz]
        at[0:ei] = g1[n * ei : (n + 1) * ei]
        if eip > ei:
            at[ei:] = jnp.zeros((eip - ei, hs_w), F32)
    hb[...] = gb_f[...].astype(BF16)
    push(10, hb.at[1 - c], cb, by(c=1 - c))

    def add_core(phase, own, got, to, out, slots):
        arrived(phase, got)
        out[...] = (own[c].astype(F32) + got[...].astype(F32)).astype(BF16)
        for d in range(1, nx):
            xd = lax.rem(x + d, nx)
            push(to, out.at[xd], slots.at[d - 1], by(x=xd))

    def add_x(phase, own, got, to, out, slots):
        arrived(phase, got)
        total = own[x].astype(F32)
        for d in range(1, nx):
            total += got[d - 1].astype(F32)
        out[...] = total.astype(BF16)
        for d in range(nz - 1, 0, -1):
            zd = lax.rem(z + d, nz)
            push(to, out.at[zd], slots.at[d - 1], by(z=zd))

    def add_z(phase, own, got):
        arrived(phase, got)
        total = own[z].astype(F32)
        for d in range(1, nz):
            total += got[d - 1].astype(F32)
        return total

    add_core(9, ha, ca, 11, xa, rxa)
    add_core(10, hb, cb, 12, xb, rxb)

    mine = pl.ds(pl.multiple_of(y * fs_w, fs_w), fs_w)
    arrived(6, rows_g)
    arrived(7, wn1_g)
    arrived(8, epg_g)
    grad_e = ge_ref[:, mine].astype(F32) + dot_t(epg, win_ref[0, mine])
    to_send = dot_t(h_hot, win_ref[1, mine])
    grad_n = (
        gn_ref[:, mine].astype(F32)
        + dot_t(npg, wn_ref[0, mine])
        + dot_t(s_hot, win_ref[1, mine])
        + dot_t(r_hot, win_ref[2, mine])
    )
    for d in range(1, ny):
        part = epg_g[d - 1]
        s_d = dot(hot_st, part).astype(BF16)
        h_d = dot(hot_ht, part).astype(BF16)
        r_d = dot(hot_rt, part).astype(BF16)
        grad_e += dot_t(part, rows_g[d - 1, 0])
        to_send += dot_t(h_d, rows_g[d - 1, 1])
        grad_n += (
            dot_t(s_d, rows_g[d - 1, 1])
            + dot_t(r_d, rows_g[d - 1, 2])
            + dot_t(npg_g[d - 1], wn1_g[d - 1])
        )
    to_send = to_send.astype(BF16)
    for d in range(nz):
        s_out[d] = to_send[d * nxc : (d + 1) * nxc]
    s_a[0] = to_send[0:nxc]
    for d in range(nz - 1, 0, -1):
        push(13, s_out.at[d], s_a.at[d], z_back(d))
    o_edges[...] = grad_e.astype(BF16)

    add_x(11, xa, rxa, 14, za, rza)
    add_x(12, xb, rxb, 15, zb, rzb)

    arrived(13, s_a.at[pl.ds(1, nz - 1)])
    r_i = iota((owners, owners), 0)
    back = hot(iota((owners, owners), 1) == (r_i % nz) * nxc + r_i // nz)
    mid = dot(back, s_a[...].reshape(owners, fs_w)).astype(BF16)
    for k in range(nxc):
        s_mid[k] = mid[k * nz : (k + 1) * nz]
    s_b[0] = mid[0:nz]
    for k in range(1, nxc):
        push(16, s_mid.at[k], s_b.at[k], xc_back(k))

    total_a = add_z(14, za, rza)
    o_ni[...] = total_a[0:ni]
    turned = jnp.transpose(total_a[ni : ni + 2 * eo])
    o_eo[...] = turned[:, 0:eo]
    o_no[...] = turned[:, eo:]
    total_b = add_z(15, zb, rzb)
    o_ei[...] = total_b[0:ei]

    arrived(16, s_b.at[pl.ds(1, nxc - 1)])
    grad_n += dot(sl_perm, s_b[...].reshape(owners, fs_w))
    o_nodes[...] = grad_n.astype(BF16)

    left(0, out1.at[pl.ds(1, nxc - 1)])
    left(1, out2.at[pl.ds(1, nz - 1)])
    left(2, wout_g)
    left(3, wn2_g)
    left(4, hs_g)
    left(5, npg_g)
    left(6, rows_g)
    left(7, wn1_g)
    left(8, epg_g)
    left(9, ca)
    left(10, cb)
    left(11, rxa)
    left(12, rxb)
    left(13, s_a.at[pl.ds(1, nz - 1)])
    left(14, rza)
    left(15, rzb)
    left(16, s_b.at[pl.ds(1, nxc - 1)])


def body(nz, nx, ny, nodes, edges, gn, ge, win, be, wout, wn, bn, wno, snd, rcv, vc, sl):
    nd, d = nodes.shape
    ed = edges.shape[0]
    hw = wout.shape[0]
    fw = d // ny
    nxc = 2 * nx
    owners = nz * nxc
    ni, eo, ei = 2 * d // owners, d // owners, 3 * d // owners
    ra = ni + 2 * eo
    rb = -(-ei // 16) * 16
    vm = pltpu.VMEM
    phases = 17
    v_spec = pl.BlockSpec(memory_space=pltpu.VMEM)
    s_spec = pl.BlockSpec(memory_space=pltpu.SMEM)
    outs = pl.pallas_call(
        functools.partial(kernel, nz, nx, ny),
        out_shape=(
            jax.ShapeDtypeStruct((nd, fw), BF16),
            jax.ShapeDtypeStruct((ed, fw), BF16),
            jax.ShapeDtypeStruct((ei, hw), F32),
            jax.ShapeDtypeStruct((hw, eo), F32),
            jax.ShapeDtypeStruct((ni, hw), F32),
            jax.ShapeDtypeStruct((hw, eo), F32),
        ),
        in_specs=[v_spec] * 3 + [s_spec] + [v_spec] * 10,
        out_specs=(v_spec,) * 6,
        scratch_shapes=[
            vm((nxc, nz, d), BF16),
            vm((nxc, nz, d), BF16),
            vm((nz, nxc, d), BF16),
            vm((nz, nxc, d), BF16),
            vm((ny - 1, hw, d), BF16),
            vm((ny - 1, d, hw), BF16),
            vm((ny - 1, 3, fw, hw), BF16),
            vm((ny - 1, fw, hw), BF16),
            vm((nd, hw), BF16),
            vm((ny - 1, nd, hw), BF16),
            vm((nd, hw), BF16),
            vm((ny - 1, nd, hw), BF16),
            vm((ed, hw), BF16),
            vm((ny - 1, ed, hw), BF16),
            vm((2, nx, nz, ra, hw), F32),
            vm((2, nx, nz, rb, hw), F32),
            vm((3 * d, hw), F32),
            vm((2 * d, hw), F32),
            vm((d, hw), F32),
            vm((d, hw), F32),
            vm((2, nx, nz, ra, hw), BF16),
            vm((2, nx, nz, rb, hw), BF16),
            vm((nx, nz, ra, hw), BF16),
            vm((nx, nz, rb, hw), BF16),
            vm((nx, nz, ra, hw), BF16),
            vm((nx, nz, rb, hw), BF16),
            vm((nx - 1, nz, ra, hw), BF16),
            vm((nx - 1, nz, rb, hw), BF16),
            vm((nz, ra, hw), BF16),
            vm((nz, rb, hw), BF16),
            vm((nz - 1, ra, hw), BF16),
            vm((nz - 1, rb, hw), BF16),
            vm((nz, nxc, fw), BF16),
            vm((nz, nxc, fw), BF16),
            vm((nxc, nz, fw), BF16),
            vm((nxc, nz, fw), BF16),
            pltpu.SemaphoreType.DMA((phases,)),
            pltpu.SemaphoreType.DMA((phases,)),
        ],
        compiler_params=pltpu.CompilerParams(collective_id=0, has_side_effects=True),
    )(
        sl.reshape(1, owners),
        snd.reshape(1, ed),
        rcv.reshape(1, ed),
        vc,
        nodes,
        edges,
        gn,
        ge,
        win.reshape(3, d, hw),
        be.reshape(1, hw),
        wout,
        wn.reshape(2, d, hw),
        bn.reshape(1, hw),
        wno,
    )
    return outs


def solution(mesh):
    ny = mesh.shape["chan"]
    nx = 4 if mesh.shape["node"] == 128 else 2
    nz = mesh.shape["node"] // (2 * nx)
    split = Mesh(mesh.devices.reshape(nz, nx, 2, ny), ("z", "x", "c", "y"))
    in_specs = (
        P(NODE, None),
        P(NODE, None),
        P(NODE, None),
        P(NODE, None),
        P(None, "y"),
        P("y"),
        P("y", None),
        P(None, "y"),
        P("y"),
        P("y", None),
        P(NODE),
        P(NODE),
        P(NODE),
        P(NODE, None),
    )
    out_specs = (
        P(NODE, "y"),
        P(NODE, "y"),
        P(NODE, "y"),
        P("y", NODE),
        P(NODE, "y"),
        P("y", NODE),
    )
    return jax.shard_map(
        functools.partial(body, nz, nx, ny),
        mesh=split,
        in_specs=in_specs,
        out_specs=out_specs,
        check_vma=False,
    )
```

```python
import functools

import jax
import jax.numpy as jnp
from jax import lax
from jax.experimental import pallas as pl
from jax.experimental.pallas import tpu as pltpu
from jax.sharding import Mesh
from jax.sharding import PartitionSpec as P

NODE = ("z", "x", "c")
MESH = pl.DeviceIdType.MESH
F32 = jnp.float32
BF16 = jnp.bfloat16


def dot(a, b):
    return jnp.dot(a, b, preferred_element_type=F32)


def dot_t(a, b):
    return lax.dot_general(a, b, (((1,), (1,)), ((), ())), preferred_element_type=F32)


def t_dot(a, b):
    return lax.dot_general(a, b, (((0,), (0,)), ((), ())), preferred_element_type=F32)


def iota(shape, dim):
    return lax.broadcasted_iota(jnp.int32, shape, dim)


def hot(cond):
    return jnp.where(cond, 1.0, 0.0).astype(BF16)


def two_parts(v):
    high = v.astype(BF16)
    return high, (v - high.astype(F32)).astype(BF16)


def sigmoid(v):
    return 1.0 / (1.0 + jnp.exp(-v))


def kernel(
    nz,
    nx,
    ny,
    sl_in,
    snd_in,
    rcv_in,
    vc_in,
    n_in,
    e_in,
    gn_in,
    ge_in,
    win_in,
    be_in,
    wout_in,
    wn_in,
    bn_in,
    wno_in,
    o_wide,
    o_rows,
    sl_ref,
    snd_ref,
    rcv_ref,
    vc_ref,
    n_ref,
    e_ref,
    gn_ref,
    ge_ref,
    win_ref,
    be_ref,
    wout_ref,
    wn_ref,
    bn_ref,
    wno_ref,
    load,
    out1,
    r1,
    out2,
    r2,
    wout_g,
    wn2_g,
    rows_g,
    wn1_g,
    hs_b,
    hs_g,
    npg_b,
    npg_g,
    epg_b,
    epg_g,
    ga_f,
    gb_f,
    g1,
    g2,
    g3,
    g4,
    ha,
    hb,
    ca,
    cb,
    xa,
    xb,
    rxa,
    rxb,
    za,
    zb,
    rza,
    rzb,
    s_out,
    s_a,
    s_mid,
    s_b,
    send,
    recv,
):
    z, x, c, y = (lax.axis_index(a) for a in ("z", "x", "c", "y"))
    nxc = 2 * nx
    owners = nz * nxc
    nd, d_feat = n_ref.shape
    ed = e_ref.shape[0]
    hs_w = wout_ref.shape[0]
    fs_w = d_feat // ny
    block = ed // vc_ref.shape[0]

    def by(**kw):
        return kw

    z_off = lambda d: by(z=lax.rem(z + d, nz))
    y_off = lambda d: by(y=lax.rem(y + d, ny))
    xc_off = lambda k: by(x=lax.rem(x + k // 2, nx), c=c if k % 2 == 0 else 1 - c)
    xc_back = lambda k: by(x=lax.rem(x + nx - k // 2, nx), c=c if k % 2 == 0 else 1 - c)
    z_back = lambda d: by(z=lax.rem(z + nz - d, nz))

    barrier = pltpu.get_barrier_semaphore()
    peers = (
        [z_off(d) for d in range(1, nz)]
        + [xc_off(k) for k in range(1, nxc)]
        + [y_off(d) for d in range(1, ny)]
    )
    for peer in peers:
        pl.semaphore_signal(barrier, inc=1, device_id=peer, device_id_type=MESH)

    sources = (sl_in, n_in, wout_in, wn_in, e_in, win_in, snd_in, rcv_in, vc_in, be_in, bn_in, ge_in, gn_in, wno_in)
    places = (sl_ref, n_ref, wout_ref, wn_ref, e_ref, win_ref, snd_ref, rcv_ref, vc_ref, be_ref, bn_ref, ge_ref, gn_ref, wno_ref)
    loads = [pltpu.make_async_copy(a, b, load.at[i]) for i, (a, b) in enumerate(zip(sources, places))]
    for copy in loads:
        copy.start()

    def push(phase, src, dst, peer):
        pltpu.make_async_remote_copy(
            src_ref=src,
            dst_ref=dst,
            send_sem=send.at[phase],
            recv_sem=recv.at[phase],
            device_id=peer,
            device_id_type=MESH,
        ).start()

    def arrived(phase, ref):
        with jax.named_scope(f"wait{phase}"):
            pltpu.make_async_copy(ref, ref, recv.at[phase]).wait()

    def left(phase, ref):
        pltpu.make_async_copy(ref, ref, send.at[phase]).wait()

    with jax.named_scope("load0"):
        for copy in loads[:2]:
            copy.wait()
    nodes = n_ref[...]
    r_q = iota((owners, owners), 1)
    k_of, dz_of = r_q // nz, r_q % nz
    q_of = (
        ((z + dz_of) & (nz - 1)) * nxc
        + ((x + (k_of >> 1)) & (nx - 1)) * 2
        + (c ^ (k_of & 1))
    )
    perm_q = hot(iota((owners, owners), 0) == q_of)
    sl_hot = hot(iota((nd, owners), 0) == sl_ref[...])
    sl_perm = dot(sl_hot, perm_q).astype(BF16)
    rows_out = t_dot(sl_perm, nodes).astype(BF16)
    for k in range(nxc):
        out1[k] = rows_out[k * nz : (k + 1) * nz]
    r1[0] = rows_out[0:nz]

    with jax.named_scope("entry"):
        pl.semaphore_wait(barrier, len(peers))

    for k in range(1, nxc):
        push(0, out1.at[k], r1.at[k], xc_off(k))
    for copy in loads[2:4]:
        copy.wait()
    for d in range(1, ny):
        push(2, wout_ref, wout_g.at[d - 1], y_off(d))
    for d in range(1, ny):
        push(3, wn_ref.at[1], wn2_g.at[d - 1], y_off(d))

    t_i = iota((owners, owners), 0)
    stage = hot(iota((owners, owners), 1) == (t_i % nxc) * nz + t_i // nxc)
    arrived(0, r1.at[pl.ds(1, nxc - 1)])
    second = dot(stage, r1[...].reshape(owners, d_feat)).astype(BF16)
    for d in range(nz):
        out2[d] = second[d * nxc : (d + 1) * nxc]
    r2[0] = second[0:nxc]
    for d in range(nz - 1, 0, -1):
        push(1, out2.at[d], r2.at[d], z_off(d))

    for copy in loads[4:]:
        copy.wait()
    snd, rcv = snd_ref[...].reshape(1, ed), rcv_ref[...].reshape(1, ed)
    t_e = iota((owners, ed), 0)
    k_t, dz_t = t_e % nxc, t_e // nxc
    p_t = (
        ((z - dz_t) & (nz - 1)) * nxc
        + ((x - (k_t >> 1)) & (nx - 1)) * 2
        + (c ^ (k_t & 1))
    )
    hot_st = hot(iota((nd, ed), 0) == snd)
    hot_ht = hot(p_t + nd == snd)
    hot_rt = hot(iota((nd, ed), 0) == rcv)

    def picked(onehot_t, table):
        high, low = two_parts(table)
        return t_dot(onehot_t, high) + t_dot(onehot_t, low)

    live = jnp.concatenate(
        [
            jnp.where(iota((block, hs_w), 0) < vc_ref[b], 1.0, 0.0)
            for b in range(ed // block)
        ],
        axis=0,
    )
    edges = e_ref[...]
    base = (
        dot(edges, win_ref[0])
        + be_ref[...]
        + picked(hot_st, dot(nodes, win_ref[1]))
        + picked(hot_rt, dot(nodes, win_ref[2]))
    )
    ge = ge_ref[...]
    wout = wout_ref[...]
    ge_w = dot_t(ge, wout)
    gn = gn_ref[...]
    gn_w = dot_t(gn, wno_ref[...])
    base_n = dot(nodes, wn_ref[0]) + bn_ref[...]

    arrived(1, r2.at[pl.ds(1, nz - 1)])
    halo = r2[...].reshape(owners, d_feat)
    pre = base + picked(hot_ht, dot(halo, win_ref[1]))
    sg = sigmoid(pre)
    hidden = (pre * sg * live).astype(BF16)
    slope = sg * (1.0 + pre * (1.0 - sg)) * live
    hs = dot(hot_rt, hidden).astype(BF16)
    hs_b[...] = hs
    for d in range(1, ny):
        push(4, hs_b, hs_g.at[d - 1], y_off(d))
    geo = t_dot(ge, hidden)
    arrived(2, wout_g)
    arrived(4, hs_g)
    agg = dot(hs, wout)
    for d in range(1, ny):
        agg += dot(hs_g[d - 1], wout_g[d - 1])
    agg = agg.astype(BF16)

    npre = base_n + dot(agg, wn_ref[1])
    nsg = sigmoid(npre)
    nhid = (npre * nsg).astype(BF16)
    npg = (gn_w * (nsg * (1.0 + npre * (1.0 - nsg)))).astype(BF16)
    npg_b[...] = npg
    for d in range(1, ny):
        push(5, npg_b, npg_g.at[d - 1], y_off(d))
    for d in range(1, ny):
        yd = pl.multiple_of(lax.rem(y + d, ny) * fs_w, fs_w)
        push(6, win_ref.at[:, pl.ds(yd, fs_w)], rows_g.at[d - 1], y_off(d))
        push(7, wn_ref.at[0, pl.ds(yd, fs_w)], wn1_g.at[d - 1], y_off(d))
    g4[...] = t_dot(gn, nhid)
    g2[0:d_feat] = t_dot(nodes, npg)
    g2[d_feat:] = t_dot(agg, npg)
    arrived(3, wn2_g)
    arrived(5, npg_g)
    grad_agg = dot_t(npg, wn_ref[1])
    for d in range(1, ny):
        grad_agg += dot_t(npg_g[d - 1], wn2_g[d - 1])
    grad_agg = grad_agg.astype(BF16)
    epg = ((ge_w + picked(hot_rt, dot_t(grad_agg, wout))) * slope).astype(BF16)
    epg_b[...] = epg
    for d in range(1, ny):
        push(8, epg_b, epg_g.at[d - 1], y_off(d))
    g3[...] = geo + t_dot(grad_agg, hs)

    ni, eo, ei = 2 * d_feat // owners, d_feat // owners, 3 * d_feat // owners
    eip = gb_f.shape[3]

    def owner(n):
        return n % 2, (n // 2) % nx, n // nxc

    for n in range(owners):
        oc, ox, oz = owner(n)
        at = ga_f.at[oc, ox, oz]
        at[0:ni] = g2[n * ni : (n + 1) * ni]
        at[ni : ni + eo] = g3[n * eo : (n + 1) * eo]
        at[ni + eo : ni + 2 * eo] = g4[n * eo : (n + 1) * eo]
    ha[...] = ga_f[...].astype(BF16)
    push(9, ha.at[1 - c], ca, by(c=1 - c))

    s_hot = dot(hot_st, epg).astype(BF16)
    h_hot = dot(hot_ht, epg).astype(BF16)
    r_hot = dot(hot_rt, epg).astype(BF16)
    g1[0:d_feat] = t_dot(edges, epg)
    g1[d_feat : 2 * d_feat] = t_dot(nodes, s_hot) + t_dot(halo, h_hot)
    g1[2 * d_feat :] = t_dot(nodes, r_hot)
    for n in range(owners):
        oc, ox, oz = owner(n)
        at = gb_f.at[oc, ox, oz]
        at[0:ei] = g1[n * ei : (n + 1) * ei]
        if eip > ei:
            at[ei:] = jnp.zeros((eip - ei, hs_w), F32)
    hb[...] = gb_f[...].astype(BF16)
    push(10, hb.at[1 - c], cb, by(c=1 - c))

    def add_core(phase, own, got, to, out, slots):
        arrived(phase, got)
        out[...] = (own[c].astype(F32) + got[...].astype(F32)).astype(BF16)
        for d in range(1, nx):
            xd = lax.rem(x + d, nx)
            push(to, out.at[xd], slots.at[d - 1], by(x=xd))

    def add_x(phase, own, got, to, out, slots):
        arrived(phase, got)
        total = own[x].astype(F32)
        for d in range(1, nx):
            total += got[d - 1].astype(F32)
        out[...] = total.astype(BF16)
        for d in range(nz - 1, 0, -1):
            zd = lax.rem(z + d, nz)
            push(to, out.at[zd], slots.at[d - 1], by(z=zd))

    def add_z(phase, own, got):
        arrived(phase, got)
        total = own[z].astype(F32)
        for d in range(1, nz):
            total += got[d - 1].astype(F32)
        return total

    add_core(9, ha, ca, 11, xa, rxa)
    add_core(10, hb, cb, 12, xb, rxb)

    mine = pl.ds(pl.multiple_of(y * fs_w, fs_w), fs_w)
    arrived(6, rows_g)
    arrived(7, wn1_g)
    arrived(8, epg_g)
    grad_e = ge_ref[:, mine].astype(F32) + dot_t(epg, win_ref[0, mine])
    to_send = dot_t(h_hot, win_ref[1, mine])
    grad_n = (
        gn_ref[:, mine].astype(F32)
        + dot_t(npg, wn_ref[0, mine])
        + dot_t(s_hot, win_ref[1, mine])
        + dot_t(r_hot, win_ref[2, mine])
    )
    for d in range(1, ny):
        part = epg_g[d - 1]
        s_d = dot(hot_st, part).astype(BF16)
        h_d = dot(hot_ht, part).astype(BF16)
        r_d = dot(hot_rt, part).astype(BF16)
        grad_e += dot_t(part, rows_g[d - 1, 0])
        to_send += dot_t(h_d, rows_g[d - 1, 1])
        grad_n += (
            dot_t(s_d, rows_g[d - 1, 1])
            + dot_t(r_d, rows_g[d - 1, 2])
            + dot_t(npg_g[d - 1], wn1_g[d - 1])
        )
    to_send = to_send.astype(BF16)
    for d in range(nz):
        s_out[d] = to_send[d * nxc : (d + 1) * nxc]
    s_a[0] = to_send[0:nxc]
    for d in range(nz - 1, 0, -1):
        push(13, s_out.at[d], s_a.at[d], z_back(d))
    o_wide[0:ed] = grad_e.astype(BF16)

    add_x(11, xa, rxa, 14, za, rza)
    add_x(12, xb, rxb, 15, zb, rzb)

    arrived(13, s_a.at[pl.ds(1, nz - 1)])
    r_i = iota((owners, owners), 0)
    back = hot(iota((owners, owners), 1) == (r_i % nz) * nxc + r_i // nz)
    mid = dot(back, s_a[...].reshape(owners, fs_w)).astype(BF16)
    for k in range(nxc):
        s_mid[k] = mid[k * nz : (k + 1) * nz]
    s_b[0] = mid[0:nz]
    for k in range(1, nxc):
        push(16, s_mid.at[k], s_b.at[k], xc_back(k))

    total_a = add_z(14, za, rza)
    o_rows[0 : ni + 2 * eo] = total_a
    total_b = add_z(15, zb, rzb)
    o_rows[ni + 2 * eo :] = total_b

    arrived(16, s_b.at[pl.ds(1, nxc - 1)])
    grad_n += dot(sl_perm, s_b[...].reshape(owners, fs_w))
    o_wide[ed:] = grad_n.astype(BF16)

    left(0, out1.at[pl.ds(1, nxc - 1)])
    left(1, out2.at[pl.ds(1, nz - 1)])
    left(2, wout_g)
    left(3, wn2_g)
    left(4, hs_g)
    left(5, npg_g)
    left(6, rows_g)
    left(7, wn1_g)
    left(8, epg_g)
    left(9, ca)
    left(10, cb)
    left(11, rxa)
    left(12, rxb)
    left(13, s_a.at[pl.ds(1, nz - 1)])
    left(14, rza)
    left(15, rzb)
    left(16, s_b.at[pl.ds(1, nxc - 1)])


def hand_out(wide, rows, o_nodes, o_edges, o_ei, o_eo, o_ni, o_no):
    ed, ni, eo, ei = o_edges.shape[0], o_ni.shape[0], o_eo.shape[0], o_ei.shape[0]
    o_edges[...] = wide[0:ed]
    o_nodes[...] = wide[ed:]
    o_ni[...] = rows[0:ni]
    o_eo[...] = rows[ni : ni + eo]
    o_no[...] = rows[ni + eo : ni + 2 * eo]
    o_ei[...] = rows[ni + 2 * eo : ni + 2 * eo + ei]


def body(nz, nx, ny, nodes, edges, gn, ge, win, be, wout, wn, bn, wno, snd, rcv, vc, sl):
    nd, d = nodes.shape
    ed = edges.shape[0]
    hw = wout.shape[0]
    fw = d // ny
    nxc = 2 * nx
    owners = nz * nxc
    ni, eo, ei = 2 * d // owners, d // owners, 3 * d // owners
    ra = ni + 2 * eo
    rb = -(-ei // 16) * 16
    vm = pltpu.VMEM
    phases = 17
    v_spec = pl.BlockSpec(memory_space=pltpu.VMEM)
    wide, rows = pl.pallas_call(
        functools.partial(kernel, nz, nx, ny),
        out_shape=(vm((ed + nd, fw), BF16), vm((ra + rb, hw), F32)),
        in_specs=[pl.BlockSpec(memory_space=pl.ANY)] * 14,
        out_specs=(v_spec,) * 2,
        scratch_shapes=[
            vm((1, owners), jnp.int32),
            vm((ed,), jnp.int32),
            vm((ed,), jnp.int32),
            pltpu.SMEM((vc.shape[0],), jnp.int32),
            vm((nd, d), BF16),
            vm((ed, d), BF16),
            vm((nd, d), BF16),
            vm((ed, d), BF16),
            vm((3, d, hw), BF16),
            vm((1, hw), F32),
            vm((hw, d), BF16),
            vm((2, d, hw), BF16),
            vm((1, hw), F32),
            vm((hw, d), BF16),
            pltpu.SemaphoreType.DMA((14,)),
            vm((nxc, nz, d), BF16),
            vm((nxc, nz, d), BF16),
            vm((nz, nxc, d), BF16),
            vm((nz, nxc, d), BF16),
            vm((ny - 1, hw, d), BF16),
            vm((ny - 1, d, hw), BF16),
            vm((ny - 1, 3, fw, hw), BF16),
            vm((ny - 1, fw, hw), BF16),
            vm((nd, hw), BF16),
            vm((ny - 1, nd, hw), BF16),
            vm((nd, hw), BF16),
            vm((ny - 1, nd, hw), BF16),
            vm((ed, hw), BF16),
            vm((ny - 1, ed, hw), BF16),
            vm((2, nx, nz, ra, hw), F32),
            vm((2, nx, nz, rb, hw), F32),
            vm((3 * d, hw), F32),
            vm((2 * d, hw), F32),
            vm((d, hw), F32),
            vm((d, hw), F32),
            vm((2, nx, nz, ra, hw), BF16),
            vm((2, nx, nz, rb, hw), BF16),
            vm((nx, nz, ra, hw), BF16),
            vm((nx, nz, rb, hw), BF16),
            vm((nx, nz, ra, hw), BF16),
            vm((nx, nz, rb, hw), BF16),
            vm((nx - 1, nz, ra, hw), BF16),
            vm((nx - 1, nz, rb, hw), BF16),
            vm((nz, ra, hw), BF16),
            vm((nz, rb, hw), BF16),
            vm((nz - 1, ra, hw), BF16),
            vm((nz - 1, rb, hw), BF16),
            vm((nz, nxc, fw), BF16),
            vm((nz, nxc, fw), BF16),
            vm((nxc, nz, fw), BF16),
            vm((nxc, nz, fw), BF16),
            pltpu.SemaphoreType.DMA((phases,)),
            pltpu.SemaphoreType.DMA((phases,)),
        ],
        compiler_params=pltpu.CompilerParams(collective_id=0, has_side_effects=True),
    )(
        sl.reshape(1, owners),
        snd,
        rcv,
        vc,
        nodes,
        edges,
        gn,
        ge,
        win.reshape(3, d, hw),
        be.reshape(1, hw),
        wout,
        wn.reshape(2, d, hw),
        bn.reshape(1, hw),
        wno,
    )
    g_nodes, g_edges, g_ei, g_eo, g_ni, g_no = pl.pallas_call(
        hand_out,
        out_shape=(
            jax.ShapeDtypeStruct((nd, fw), BF16),
            jax.ShapeDtypeStruct((ed, fw), BF16),
            jax.ShapeDtypeStruct((ei, hw), F32),
            jax.ShapeDtypeStruct((eo, hw), F32),
            jax.ShapeDtypeStruct((ni, hw), F32),
            jax.ShapeDtypeStruct((eo, hw), F32),
        ),
        in_specs=[v_spec] * 2,
        out_specs=(v_spec,) * 6,
    )(*(pltpu.with_memory_space_constraint(v, pltpu.VMEM) for v in (wide, rows)))
    return g_nodes, g_edges, g_ei, g_eo.T, g_ni, g_no.T


def solution(mesh):
    ny = mesh.shape["chan"]
    nx = 4 if mesh.shape["node"] == 128 else 2
    nz = mesh.shape["node"] // (2 * nx)
    split = Mesh(mesh.devices.reshape(nz, nx, 2, ny), ("z", "x", "c", "y"))
    in_specs = (
        P(NODE, None),
        P(NODE, None),
        P(NODE, None),
        P(NODE, None),
        P(None, "y"),
        P("y"),
        P("y", None),
        P(None, "y"),
        P("y"),
        P("y", None),
        P(NODE),
        P(NODE),
        P(NODE),
        P(NODE, None),
    )
    out_specs = (
        P(NODE, "y"),
        P(NODE, "y"),
        P(NODE, "y"),
        P("y", NODE),
        P(NODE, "y"),
        P("y", NODE),
    )
    return jax.shard_map(
        functools.partial(body, nz, nx, ny),
        mesh=split,
        in_specs=in_specs,
        out_specs=out_specs,
        check_vma=False,
    )
```

```python
import functools

import jax
import jax.numpy as jnp
from jax import lax
from jax.experimental import pallas as pl
from jax.experimental.pallas import tpu as pltpu
from jax.sharding import Mesh
from jax.sharding import PartitionSpec as P

NODE = ("z", "x", "c")
MESH = pl.DeviceIdType.MESH
F32 = jnp.float32
BF16 = jnp.bfloat16


def dot(a, b):
    return jnp.dot(a, b, preferred_element_type=F32)


def dot_t(a, b):
    return lax.dot_general(a, b, (((1,), (1,)), ((), ())), preferred_element_type=F32)


def t_dot(a, b):
    return lax.dot_general(a, b, (((0,), (0,)), ((), ())), preferred_element_type=F32)


def iota(shape, dim):
    return lax.broadcasted_iota(jnp.int32, shape, dim)


def hot(cond):
    return jnp.where(cond, 1.0, 0.0).astype(BF16)


def two_parts(v):
    high = v.astype(BF16)
    return high, (v - high.astype(F32)).astype(BF16)


def sigmoid(v):
    return 1.0 / (1.0 + jnp.exp(-v))


PHASES = (
    "halo",
    "raw1",
    "raw2",
    "wout",
    "wout_c",
    "wn2",
    "wn2_c",
    "nb",
    "rows",
    "rows_c",
    "wn1",
    "wn1_c",
    "hs",
    "epg",
    "core_a",
    "core_b",
    "x_a",
    "x_b",
    "z_a",
    "z_b",
    "back",
    "sums",
)


def kernel(
    nz,
    nx,
    ny,
    sl_in,
    snd_in,
    rcv_in,
    vc_in,
    n_in,
    e_in,
    gn_in,
    ge_in,
    win_in,
    be_in,
    wout_in,
    wn_in,
    bn_in,
    wno_in,
    o_wide,
    o_rows,
    sl_ref,
    snd_ref,
    rcv_ref,
    vc_ref,
    n_ref,
    e_ref,
    gn_ref,
    ge_ref,
    win_ref,
    be_ref,
    wout_ref,
    wn_ref,
    bn_ref,
    wno_ref,
    load,
    p_out,
    p_in,
    out1,
    r1,
    out2,
    r2,
    wout_g,
    wn2_g,
    rows_g,
    wn1_g,
    nb_b,
    nb_g,
    hs_b,
    hs_g,
    epg_b,
    epg_g,
    ga_f,
    gb_f,
    g1,
    g2,
    g3,
    g4,
    ha,
    hb,
    ca,
    cb,
    xa,
    xb,
    rxa,
    rxb,
    za,
    zb,
    rza,
    rzb,
    back_out,
    back_in,
    sums_b,
    sums_g,
    send,
    recv,
):
    z, x, c, y = (lax.axis_index(a) for a in ("z", "x", "c", "y"))
    nxc = 2 * nx
    owners = nz * nxc
    nd, d_feat = n_ref.shape
    ed = e_ref.shape[0]
    hs_w = wout_ref.shape[0]
    fs_w = d_feat // ny
    block = ed // vc_ref.shape[0]

    def by(**kw):
        return kw

    def at_xc(k, sign=1):
        place = {}
        if k // 2:
            place["x"] = lax.rem(x + nx + sign * (k // 2), nx)
        if k % 2:
            place["c"] = 1 - c
        return place

    def at_z(d, sign=1):
        return {"z": lax.rem(z + nz + sign * d, nz)} if d else {}

    def at_y(d):
        return {"y": lax.rem(y + d, ny)}

    def hops(k, d):
        return min(d, nz - d) + min(k // 2, nx - k // 2)

    everyone = [(k, d) for k in range(nxc) for d in range(nz) if k or d]
    everyone.sort(key=lambda kd: -hops(*kd))

    sources = (sl_in, n_in, win_in, wout_in, wn_in, e_in, snd_in, rcv_in, vc_in, be_in, bn_in, ge_in, gn_in, wno_in)
    places = (sl_ref, n_ref, win_ref, wout_ref, wn_ref, e_ref, snd_ref, rcv_ref, vc_ref, be_ref, bn_ref, ge_ref, gn_ref, wno_ref)
    loads = [pltpu.make_async_copy(a, b, load.at[i]) for i, (a, b) in enumerate(zip(sources, places))]

    barrier = pltpu.get_barrier_semaphore()
    peers = [at_xc(k) | at_z(d) for k, d in everyone] + [at_y(d) for d in range(1, ny)]
    for peer in peers:
        pl.semaphore_signal(barrier, inc=1, device_id=peer, device_id_type=MESH)
    for copy in loads:
        copy.start()

    def push(phase, src, dst, peer):
        pltpu.make_async_remote_copy(
            src_ref=src,
            dst_ref=dst,
            send_sem=send.at[PHASES.index(phase)],
            recv_sem=recv.at[PHASES.index(phase)],
            device_id=peer,
            device_id_type=MESH,
        ).start()

    def arrived(phase, ref):
        with jax.named_scope(f"wait_{phase}"):
            pltpu.make_async_copy(ref, ref, recv.at[PHASES.index(phase)]).wait()

    def left(phase, ref):
        pltpu.make_async_copy(ref, ref, send.at[PHASES.index(phase)]).wait()

    with jax.named_scope("load0"):
        for copy in loads[:2]:
            copy.wait()
    nodes = n_ref[...]
    r_q = iota((owners, owners), 1)
    k_of, dz_of = r_q // nz, r_q % nz
    q_of = (
        ((z + dz_of) & (nz - 1)) * nxc
        + ((x + (k_of >> 1)) & (nx - 1)) * 2
        + (c ^ (k_of & 1))
    )
    perm_q = hot(iota((owners, owners), 0) == q_of)
    sl_hot = hot(iota((nd, owners), 0) == sl_ref[...])
    sl_perm = dot(sl_hot, perm_q).astype(BF16)
    rows_out = t_dot(sl_perm, nodes).astype(BF16)
    for copy in loads[2:3]:
        copy.wait()
    p_out[...] = dot(rows_out, win_ref[1]).reshape(owners, 1, hs_w)
    p_in[0] = p_out[0]
    for k in range(nxc):
        out1[k] = rows_out[k * nz : (k + 1) * nz]
    r1[0] = rows_out[0:nz]

    with jax.named_scope("entry"):
        pl.semaphore_wait(barrier, len(peers))

    for k, d in everyone:
        push("halo", p_out.at[k * nz + d], p_in.at[k * nz + d], at_xc(k) | at_z(d))
    for k in range(1, nxc):
        push("raw1", out1.at[k], r1.at[k], at_xc(k))

    hw2, dw2, fw2 = hs_w // 2, d_feat // 2, fs_w // 2
    for copy in loads[3:5]:
        copy.wait()
    for d in range(1, ny):
        push("wout", wout_ref.at[pl.ds(c * hw2, hw2)], wout_g.at[d - 1, c], at_y(d))
    for d in range(1, ny):
        push("wn2", wn_ref.at[1, pl.ds(c * dw2, dw2)], wn2_g.at[d - 1, c], at_y(d))

    def hand_on(phase, buf):
        arrived(phase, buf.at[:, c])
        for d in range(1, ny):
            push(phase + "_c", buf.at[d - 1, c], buf.at[d - 1, c], {"c": 1 - c})

    for copy in loads[5:]:
        copy.wait()
    gn = gn_ref[...]
    gn_w = dot_t(gn, wno_ref[...])
    base_n = dot(nodes, wn_ref[0]) + bn_ref[...]
    nb_b[0] = gn_w.astype(BF16)
    nb_b[1] = base_n.astype(BF16)
    for d in range(1, ny):
        push("nb", nb_b, nb_g.at[d - 1], at_y(d))

    snd, rcv = snd_ref[...].reshape(1, ed), rcv_ref[...].reshape(1, ed)

    def remote(k, dz):
        owner_of = (
            ((z - dz) & (nz - 1)) * nxc
            + ((x - (k >> 1)) & (nx - 1)) * 2
            + (c ^ (k & 1))
        )
        return hot(owner_of + nd == snd)

    t_e = iota((owners, ed), 0)
    hot_pt = remote(t_e // nz, t_e % nz)
    hot_ht = remote(t_e % nxc, t_e // nxc)
    hot_st = hot(iota((nd, ed), 0) == snd)
    hot_rt = hot(iota((nd, ed), 0) == rcv)

    def picked(onehot_t, table):
        high, low = two_parts(table)
        return t_dot(onehot_t, high) + t_dot(onehot_t, low)

    live = jnp.concatenate(
        [
            jnp.where(iota((block, hs_w), 0) < vc_ref[b], 1.0, 0.0)
            for b in range(ed // block)
        ],
        axis=0,
    )
    edges = e_ref[...]
    base = (
        dot(edges, win_ref[0])
        + be_ref[...]
        + picked(hot_st, dot(nodes, win_ref[1]))
        + picked(hot_rt, dot(nodes, win_ref[2]))
    )
    ge = ge_ref[...]
    wout = wout_ref[...]
    ge_w = dot_t(ge, wout)

    t_i = iota((owners, owners), 0)
    stage = hot(iota((owners, owners), 1) == (t_i % nxc) * nz + t_i // nxc)
    arrived("raw1", r1.at[pl.ds(1, nxc - 1)])
    second = dot(stage, r1[...].reshape(owners, d_feat)).astype(BF16)
    for d in range(nz):
        out2[d] = second[d * nxc : (d + 1) * nxc]
    r2[0] = second[0:nxc]
    for d in range(nz - 1, 0, -1):
        push("raw2", out2.at[d], r2.at[d], at_z(d))
    hand_on("wout", wout_g)

    arrived("halo", p_in.at[pl.ds(1, owners - 1)])
    pre = base + picked(hot_pt, p_in[...].reshape(owners, hs_w))
    sg = sigmoid(pre)
    hidden = (pre * sg * live).astype(BF16)
    slope = sg * (1.0 + pre * (1.0 - sg)) * live
    hs = dot(hot_rt, hidden).astype(BF16)
    hs_b[...] = hs
    for d in range(1, ny):
        push("hs", hs_b, hs_g.at[d - 1], at_y(d))
    hand_on("wn2", wn2_g)
    geo = t_dot(ge, hidden)
    wn2 = wn_ref[1]
    arrived("wout_c", wout_g.at[:, 1 - c])
    arrived("hs", hs_g)
    for d in range(1, ny):
        yd = pl.multiple_of(lax.rem(y + d, ny) * fs_w + c * fw2, fw2)
        push("rows", win_ref.at[:, pl.ds(yd, fw2)], rows_g.at[d - 1, c], at_y(d))
        push("wn1", wn_ref.at[0, pl.ds(yd, fw2)], wn1_g.at[d - 1, c], at_y(d))
    agg = dot(hs, wout)
    for d in range(1, ny):
        agg += dot(hs_g[d - 1], wout_g[d - 1].reshape(hs_w, d_feat))
    agg = agg.astype(BF16)

    arrived("wn2_c", wn2_g.at[:, 1 - c])
    arrived("nb", nb_g)

    def unit_grad(before, gradient, weight):
        npre = before + dot(agg, weight)
        nsg = sigmoid(npre)
        slope = nsg * (1.0 + npre * (1.0 - nsg))
        return npre * nsg, (gradient * slope).astype(BF16)

    nhid, npg = unit_grad(base_n, gn_w, wn2)
    nhid = nhid.astype(BF16)
    npgs = [npg]
    grad_agg = dot_t(npg, wn2)
    for d in range(1, ny):
        weight = wn2_g[d - 1].reshape(d_feat, hs_w)
        _, other = unit_grad(
            nb_g[d - 1, 1].astype(F32), nb_g[d - 1, 0].astype(F32), weight
        )
        npgs.append(other)
        grad_agg += dot_t(other, weight)
    grad_agg = grad_agg.astype(BF16)

    ni, eo, ei = 2 * d_feat // owners, d_feat // owners, 3 * d_feat // owners

    def owner(n):
        return n % 2, (n // 2) % nx, n // nxc

    def for_owners(blocks, sources, out):
        rows = sum(size for size, _ in sources)
        for n in range(owners):
            oc, ox, oz = owner(n)
            at, start = blocks.at[oc, ox, oz], 0
            for size, source in sources:
                at[start : start + size] = source[n * size : (n + 1) * size]
                start += size
            if rows < blocks.shape[3]:
                at[rows:] = jnp.zeros((blocks.shape[3] - rows, hs_w), F32)
        out[...] = blocks[...].astype(BF16)

    g4[...] = t_dot(gn, nhid)
    g2[0:d_feat] = t_dot(nodes, npg)
    g2[d_feat:] = t_dot(agg, npg)
    for_owners(ga_f, ((ni, g2), (eo, g4)), ha)
    push("core_a", ha.at[1 - c], ca, {"c": 1 - c})

    epg = ((ge_w + picked(hot_rt, dot_t(grad_agg, wout))) * slope).astype(BF16)
    epg_b[...] = epg
    for d in range(1, ny):
        push("epg", epg_b, epg_g.at[d - 1], at_y(d))

    def add_core(phase, own, got, to, out, slots):
        arrived(phase, got)
        out[...] = (own[c].astype(F32) + got[...].astype(F32)).astype(BF16)
        for d in range(1, nx):
            xd = lax.rem(x + d, nx)
            push(to, out.at[xd], slots.at[d - 1], {"x": xd})

    def add_x(phase, own, got, to, out, slots):
        arrived(phase, got)
        total = own[x].astype(F32)
        for d in range(1, nx):
            total += got[d - 1].astype(F32)
        out[...] = total.astype(BF16)
        for d in range(nz - 1, 0, -1):
            zd = lax.rem(z + d, nz)
            push(to, out.at[zd], slots.at[d - 1], {"z": zd})

    def add_z(phase, own, got):
        arrived(phase, got)
        total = own[z].astype(F32)
        for d in range(1, nz):
            total += got[d - 1].astype(F32)
        return total

    add_core("core_a", ha, ca, "x_a", xa, rxa)

    s_sum = dot(hot_st, epg)
    s_hot = s_sum.astype(BF16)
    h_hot = dot(hot_ht, epg).astype(BF16)
    r_hot = dot(hot_rt, epg).astype(BF16)
    g3[...] = geo + t_dot(grad_agg, hs)
    g1[0:d_feat] = t_dot(edges, epg)
    g1[2 * d_feat :] = t_dot(nodes, r_hot)
    arrived("raw2", r2.at[pl.ds(1, nz - 1)])
    halo = r2[...].reshape(owners, d_feat)
    g1[d_feat : 2 * d_feat] = t_dot(nodes, s_hot) + t_dot(halo, h_hot)
    for_owners(gb_f, ((ei, g1), (eo, g3)), hb)
    push("core_b", hb.at[1 - c], cb, {"c": 1 - c})

    back_out[...] = dot(hot_pt, epg).reshape(owners, 1, hs_w)
    back_in[0] = back_out[0]
    for k, d in everyone:
        at = k * nz + d
        push("back", back_out.at[at], back_in.at[at], at_xc(k, -1) | at_z(d, -1))
    add_core("core_b", hb, cb, "x_b", xb, rxb)
    hand_on("rows", rows_g)
    hand_on("wn1", wn1_g)

    mine = pl.ds(pl.multiple_of(y * fs_w, fs_w), fs_w)
    arrived("epg", epg_g)
    arrived("rows_c", rows_g.at[:, 1 - c])
    arrived("wn1_c", wn1_g.at[:, 1 - c])
    w_s = [win_ref[1, mine]]
    grad_e = ge_ref[:, mine].astype(F32) + dot_t(epg, win_ref[0, mine])
    grad_n = (
        gn_ref[:, mine].astype(F32)
        + dot_t(npg, wn_ref[0, mine])
        + dot_t(r_hot, win_ref[2, mine])
    )
    for d in range(1, ny):
        part = epg_g[d - 1]
        r_d = dot(hot_rt, part).astype(BF16)
        w_e, w_sender, w_r = (
            jnp.concatenate([rows_g[d - 1, 0, b], rows_g[d - 1, 1, b]], axis=0)
            for b in range(3)
        )
        w_s.append(w_sender)
        grad_e += dot_t(part, w_e)
        grad_n += dot_t(r_d, w_r) + dot_t(npgs[d], wn1_g[d - 1].reshape(fs_w, hs_w))
    o_wide[0:ed] = grad_e.astype(BF16)

    add_x("x_a", xa, rxa, "z_a", za, rza)
    add_x("x_b", xb, rxb, "z_b", zb, rzb)

    arrived("back", back_in.at[pl.ds(1, owners - 1)])
    high, low = two_parts(back_in[...].reshape(owners, hs_w))
    sums = (s_sum + dot(sl_perm, high) + dot(sl_perm, low)).astype(BF16)
    sums_b[...] = sums
    for d in range(1, ny):
        push("sums", sums_b, sums_g.at[d - 1], at_y(d))
    total_a = add_z("z_a", za, rza)
    o_rows[0 : total_a.shape[0]] = total_a
    grad_n += dot_t(sums, w_s[0])
    arrived("sums", sums_g)
    for d in range(1, ny):
        grad_n += dot_t(sums_g[d - 1], w_s[d])
    o_wide[ed:] = grad_n.astype(BF16)
    total_b = add_z("z_b", zb, rzb)
    o_rows[total_a.shape[0] :] = total_b

    left("halo", p_in.at[pl.ds(1, owners - 1)])
    left("raw1", out1.at[pl.ds(1, nxc - 1)])
    left("raw2", out2.at[pl.ds(1, nz - 1)])
    for phase, buf in (
        ("wout", wout_g),
        ("wn2", wn2_g),
        ("rows", rows_g),
        ("wn1", wn1_g),
    ):
        left(phase, buf.at[:, c])
        left(phase + "_c", buf.at[:, c])
    left("nb", nb_g)
    left("hs", hs_g)
    left("epg", epg_g)
    left("core_a", ca)
    left("core_b", cb)
    left("x_a", rxa)
    left("x_b", rxb)
    left("z_a", rza)
    left("z_b", rzb)
    left("back", back_in.at[pl.ds(1, owners - 1)])
    left("sums", sums_g)


def hand_out(wide, rows, o_nodes, o_edges, o_ei, o_eo, o_ni, o_no):
    ed, ni, eo, ei = o_edges.shape[0], o_ni.shape[0], o_eo.shape[0], o_ei.shape[0]
    second = rows.shape[0] - ei - eo
    o_edges[...] = wide[0:ed]
    o_nodes[...] = wide[ed:]
    o_ni[...] = rows[0:ni]
    o_no[...] = rows[ni : ni + eo]
    o_ei[...] = rows[second : second + ei]
    o_eo[...] = rows[second + ei :]


def body(nz, nx, ny, nodes, edges, gn, ge, win, be, wout, wn, bn, wno, snd, rcv, vc, sl):
    nd, d = nodes.shape
    ed = edges.shape[0]
    hw = wout.shape[0]
    fw = d // ny
    nxc = 2 * nx
    owners = nz * nxc
    ni, eo, ei = 2 * d // owners, d // owners, 3 * d // owners
    ra = -(-(ni + eo) // 16) * 16
    rb = ei + eo
    vm = pltpu.VMEM
    phases = len(PHASES)
    v_spec = pl.BlockSpec(memory_space=pltpu.VMEM)
    wide, rows = pl.pallas_call(
        functools.partial(kernel, nz, nx, ny),
        out_shape=(vm((ed + nd, fw), BF16), vm((ra + rb, hw), F32)),
        in_specs=[pl.BlockSpec(memory_space=pl.ANY)] * 14,
        out_specs=(v_spec,) * 2,
        scratch_shapes=[
            vm((1, owners), jnp.int32),
            vm((ed,), jnp.int32),
            vm((ed,), jnp.int32),
            pltpu.SMEM((vc.shape[0],), jnp.int32),
            vm((nd, d), BF16),
            vm((ed, d), BF16),
            vm((nd, d), BF16),
            vm((ed, d), BF16),
            vm((3, d, hw), BF16),
            vm((1, hw), F32),
            vm((hw, d), BF16),
            vm((2, d, hw), BF16),
            vm((1, hw), F32),
            vm((hw, d), BF16),
            pltpu.SemaphoreType.DMA((14,)),
            vm((owners, 1, hw), F32),
            vm((owners, 1, hw), F32),
            vm((nxc, nz, d), BF16),
            vm((nxc, nz, d), BF16),
            vm((nz, nxc, d), BF16),
            vm((nz, nxc, d), BF16),
            vm((ny - 1, 2, hw // 2, d), BF16),
            vm((ny - 1, 2, d // 2, hw), BF16),
            vm((ny - 1, 2, 3, fw // 2, hw), BF16),
            vm((ny - 1, 2, fw // 2, hw), BF16),
            vm((2, nd, hw), BF16),
            vm((ny - 1, 2, nd, hw), BF16),
            vm((nd, hw), BF16),
            vm((ny - 1, nd, hw), BF16),
            vm((ed, hw), BF16),
            vm((ny - 1, ed, hw), BF16),
            vm((2, nx, nz, ra, hw), F32),
            vm((2, nx, nz, rb, hw), F32),
            vm((3 * d, hw), F32),
            vm((2 * d, hw), F32),
            vm((d, hw), F32),
            vm((d, hw), F32),
            vm((2, nx, nz, ra, hw), BF16),
            vm((2, nx, nz, rb, hw), BF16),
            vm((nx, nz, ra, hw), BF16),
            vm((nx, nz, rb, hw), BF16),
            vm((nx, nz, ra, hw), BF16),
            vm((nx, nz, rb, hw), BF16),
            vm((nx - 1, nz, ra, hw), BF16),
            vm((nx - 1, nz, rb, hw), BF16),
            vm((nz, ra, hw), BF16),
            vm((nz, rb, hw), BF16),
            vm((nz - 1, ra, hw), BF16),
            vm((nz - 1, rb, hw), BF16),
            vm((owners, 1, hw), F32),
            vm((owners, 1, hw), F32),
            vm((nd, hw), BF16),
            vm((ny - 1, nd, hw), BF16),
            pltpu.SemaphoreType.DMA((phases,)),
            pltpu.SemaphoreType.DMA((phases,)),
        ],
        compiler_params=pltpu.CompilerParams(collective_id=0, has_side_effects=True),
    )(
        sl.reshape(1, owners),
        snd,
        rcv,
        vc,
        nodes,
        edges,
        gn,
        ge,
        win.reshape(3, d, hw),
        be.reshape(1, hw),
        wout,
        wn.reshape(2, d, hw),
        bn.reshape(1, hw),
        wno,
    )
    g_nodes, g_edges, g_ei, g_eo, g_ni, g_no = pl.pallas_call(
        hand_out,
        out_shape=(
            jax.ShapeDtypeStruct((nd, fw), BF16),
            jax.ShapeDtypeStruct((ed, fw), BF16),
            jax.ShapeDtypeStruct((ei, hw), F32),
            jax.ShapeDtypeStruct((eo, hw), F32),
            jax.ShapeDtypeStruct((ni, hw), F32),
            jax.ShapeDtypeStruct((eo, hw), F32),
        ),
        in_specs=[v_spec] * 2,
        out_specs=(v_spec,) * 6,
    )(*(pltpu.with_memory_space_constraint(v, pltpu.VMEM) for v in (wide, rows)))
    return g_nodes, g_edges, g_ei, g_eo.T, g_ni, g_no.T


def solution(mesh):
    ny = mesh.shape["chan"]
    nx = 4 if mesh.shape["node"] == 128 else 2
    nz = mesh.shape["node"] // (2 * nx)
    split = Mesh(mesh.devices.reshape(nz, nx, 2, ny), ("z", "x", "c", "y"))
    in_specs = (
        P(NODE, None),
        P(NODE, None),
        P(NODE, None),
        P(NODE, None),
        P(None, "y"),
        P("y"),
        P("y", None),
        P(None, "y"),
        P("y"),
        P("y", None),
        P(NODE),
        P(NODE),
        P(NODE),
        P(NODE, None),
    )
    out_specs = (
        P(NODE, "y"),
        P(NODE, "y"),
        P(NODE, "y"),
        P("y", NODE),
        P(NODE, "y"),
        P("y", NODE),
    )
    return jax.shard_map(
        functools.partial(body, nz, nx, ny),
        mesh=split,
        in_specs=in_specs,
        out_specs=out_specs,
        check_vma=False,
    )
```

```python
import functools

import jax
import jax.numpy as jnp
from jax import lax
from jax.experimental import pallas as pl
from jax.experimental.pallas import tpu as pltpu
from jax.sharding import Mesh
from jax.sharding import PartitionSpec as P

NODE = ("z", "x", "c")
MESH = pl.DeviceIdType.MESH
F32 = jnp.float32
BF16 = jnp.bfloat16


def dot(a, b):
    return jnp.dot(a, b, preferred_element_type=F32)


def dot_t(a, b):
    return lax.dot_general(a, b, (((1,), (1,)), ((), ())), preferred_element_type=F32)


def t_dot(a, b):
    return lax.dot_general(a, b, (((0,), (0,)), ((), ())), preferred_element_type=F32)


def iota(shape, dim):
    return lax.broadcasted_iota(jnp.int32, shape, dim)


def hot(cond):
    return jnp.where(cond, 1.0, 0.0).astype(BF16)


def two_parts(v):
    high = v.astype(BF16)
    return high, (v - high.astype(F32)).astype(BF16)


def sigmoid(v):
    return 1.0 / (1.0 + jnp.exp(-v))


PHASES = (
    "halo",
    "raw1",
    "raw2",
    "wout",
    "wout_c",
    "wn2",
    "wn2_c",
    "nb",
    "rows",
    "rows_c",
    "wn1",
    "wn1_c",
    "hs",
    "epg",
    "core_a",
    "core_b",
    "x_a",
    "x_b",
    "z_a",
    "z_b",
    "back",
    "sums",
)


def kernel(
    nz,
    nx,
    ny,
    sl_in,
    snd_in,
    rcv_in,
    vc_in,
    n_in,
    e_in,
    gn_in,
    ge_in,
    win_in,
    be_in,
    wout_in,
    wn_in,
    bn_in,
    wno_in,
    o_wide,
    o_rows,
    sl_ref,
    snd_ref,
    rcv_ref,
    vc_ref,
    n_ref,
    e_ref,
    gn_ref,
    ge_ref,
    win_ref,
    be_ref,
    wout_ref,
    wn_ref,
    bn_ref,
    wno_ref,
    load,
    p_out,
    p_in,
    out1,
    r1,
    out2,
    r2,
    wout_g,
    wn2_g,
    rows_g,
    wn1_g,
    nb_b,
    nb_g,
    hs_b,
    hs_g,
    epg_b,
    epg_g,
    ga_f,
    gb_f,
    g1,
    g2,
    g3,
    g4,
    ha,
    hb,
    ca,
    cb,
    xa,
    xb,
    rxa,
    rxb,
    za,
    zb,
    rza,
    rzb,
    back_out,
    back_in,
    sums_b,
    sums_g,
    hot_p,
    hot_r,
    n_t,
    gn_t,
    e_t,
    send,
    recv,
):
    z, x, c, y = (lax.axis_index(a) for a in ("z", "x", "c", "y"))
    nxc = 2 * nx
    owners = nz * nxc
    nd, d_feat = n_ref.shape
    ed = e_ref.shape[0]
    hs_w = wout_ref.shape[0]
    fs_w = d_feat // ny
    block = ed // vc_ref.shape[0]

    def by(**kw):
        return kw

    def at_xc(k, sign=1):
        place = {}
        if k // 2:
            place["x"] = lax.rem(x + nx + sign * (k // 2), nx)
        if k % 2:
            place["c"] = 1 - c
        return place

    def at_z(d, sign=1):
        return {"z": lax.rem(z + nz + sign * d, nz)} if d else {}

    def at_y(d):
        return {"y": lax.rem(y + d, ny)}

    def hops(k, d):
        return min(d, nz - d) + min(k // 2, nx - k // 2)

    def far_first(n):
        return sorted(range(1, n), key=lambda d: -min(d, n - d))

    everyone = [(k, d) for k in range(nxc) for d in range(nz) if k or d]
    everyone.sort(key=lambda kd: -hops(*kd))

    sources = (sl_in, n_in, win_in, wout_in, wn_in, e_in, snd_in, rcv_in, vc_in, be_in, bn_in, ge_in, gn_in, wno_in)
    places = (sl_ref, n_ref, win_ref, wout_ref, wn_ref, e_ref, snd_ref, rcv_ref, vc_ref, be_ref, bn_ref, ge_ref, gn_ref, wno_ref)
    loads = [pltpu.make_async_copy(a, b, load.at[i]) for i, (a, b) in enumerate(zip(sources, places))]

    barrier = pltpu.get_barrier_semaphore()
    peers = [at_xc(k) | at_z(d) for k, d in everyone] + [at_y(d) for d in range(1, ny)]
    for peer in peers:
        pl.semaphore_signal(barrier, inc=1, device_id=peer, device_id_type=MESH)
    for copy in loads:
        copy.start()

    def push(phase, src, dst, peer):
        pltpu.make_async_remote_copy(
            src_ref=src,
            dst_ref=dst,
            send_sem=send.at[PHASES.index(phase)],
            recv_sem=recv.at[PHASES.index(phase)],
            device_id=peer,
            device_id_type=MESH,
        ).start()

    def arrived(phase, ref):
        with jax.named_scope(f"wait_{phase}"):
            pltpu.make_async_copy(ref, ref, recv.at[PHASES.index(phase)]).wait()

    def left(phase, ref):
        pltpu.make_async_copy(ref, ref, send.at[PHASES.index(phase)]).wait()

    with jax.named_scope("load0"):
        for copy in loads[:2]:
            copy.wait()
    nodes = n_ref[...]
    r_q = iota((owners, owners), 1)
    k_of, dz_of = r_q // nz, r_q % nz
    q_of = (
        ((z + dz_of) & (nz - 1)) * nxc
        + ((x + (k_of >> 1)) & (nx - 1)) * 2
        + (c ^ (k_of & 1))
    )
    perm_q = hot(iota((owners, owners), 0) == q_of)
    sl_hot = hot(iota((nd, owners), 0) == sl_ref[...])
    sl_perm = dot(sl_hot, perm_q).astype(BF16)
    rows_out = t_dot(sl_perm, nodes).astype(BF16)
    for copy in loads[2:3]:
        copy.wait()
    p_out[...] = dot(rows_out, win_ref[1]).reshape(owners, 1, hs_w)
    p_in[0] = p_out[0]
    for k in range(nxc):
        out1[k] = rows_out[k * nz : (k + 1) * nz]
    r1[0] = rows_out[0:nz]

    with jax.named_scope("entry"):
        pl.semaphore_wait(barrier, len(peers))

    for k, d in everyone:
        push("halo", p_out.at[k * nz + d], p_in.at[k * nz + d], at_xc(k) | at_z(d))
    for k in range(1, nxc):
        push("raw1", out1.at[k], r1.at[k], at_xc(k))

    hw2, dw2, fw2 = hs_w // 2, d_feat // 2, fs_w // 2
    for copy in loads[3:5]:
        copy.wait()
    for d in far_first(ny):
        push("wout", wout_ref.at[pl.ds(c * hw2, hw2)], wout_g.at[d - 1, c], at_y(d))
    for d in far_first(ny):
        push("wn2", wn_ref.at[1, pl.ds(c * dw2, dw2)], wn2_g.at[d - 1, c], at_y(d))

    def hand_on(phase, buf):
        arrived(phase, buf.at[:, c])
        for d in far_first(ny):
            push(phase + "_c", buf.at[d - 1, c], buf.at[d - 1, c], {"c": 1 - c})

    for copy in loads[5:]:
        copy.wait()
    gn = gn_ref[...]
    gn_w = dot_t(gn, wno_ref[...])
    base_n = dot(nodes, wn_ref[0]) + bn_ref[...]
    nb_b[0] = gn_w.astype(BF16)
    nb_b[1] = base_n.astype(BF16)
    for d in far_first(ny):
        push("nb", nb_b, nb_g.at[d - 1], at_y(d))

    snd, rcv = snd_ref[...].reshape(1, ed), rcv_ref[...].reshape(1, ed)

    def remote(k, dz):
        owner_of = (
            ((z - dz) & (nz - 1)) * nxc
            + ((x - (k >> 1)) & (nx - 1)) * 2
            + (c ^ (k & 1))
        )
        return hot(owner_of + nd == snd)

    t_e = iota((owners, ed), 0)
    hot_pt = remote(t_e // nz, t_e % nz)
    hot_ht = remote(t_e % nxc, t_e // nxc)
    hot_st = hot(iota((nd, ed), 0) == snd)
    hot_rt = hot(iota((nd, ed), 0) == rcv)

    def picked(onehot, table):
        high, low = two_parts(table)
        return dot(onehot, high) + dot(onehot, low)

    hot_p[...] = jnp.transpose(hot_pt)
    hot_r[...] = jnp.transpose(hot_rt)

    live = jnp.concatenate(
        [
            jnp.where(iota((block, hs_w), 0) < vc_ref[b], 1.0, 0.0)
            for b in range(ed // block)
        ],
        axis=0,
    )
    edges = e_ref[...]
    base = (
        dot(edges, win_ref[0])
        + be_ref[...]
        + picked(jnp.transpose(hot_st), dot(nodes, win_ref[1]))
        + picked(hot_r[...], dot(nodes, win_ref[2]))
    )
    ge = ge_ref[...]
    wout = wout_ref[...]
    ge_w = dot_t(ge, wout)

    n_t[...] = jnp.transpose(nodes)
    gn_t[...] = jnp.transpose(gn)
    e_t[...] = jnp.transpose(edges)

    t_i = iota((owners, owners), 0)
    stage = hot(iota((owners, owners), 1) == (t_i % nxc) * nz + t_i // nxc)
    arrived("raw1", r1.at[pl.ds(1, nxc - 1)])
    second = dot(stage, r1[...].reshape(owners, d_feat)).astype(BF16)
    for d in range(nz):
        out2[d] = second[d * nxc : (d + 1) * nxc]
    r2[0] = second[0:nxc]
    for d in far_first(nz):
        push("raw2", out2.at[d], r2.at[d], at_z(d))
    hand_on("wout", wout_g)

    arrived("halo", p_in.at[pl.ds(1, owners - 1)])
    pre = base + picked(hot_p[...], p_in[...].reshape(owners, hs_w))
    sg = sigmoid(pre)
    hidden = (pre * sg * live).astype(BF16)
    slope = sg * (1.0 + pre * (1.0 - sg)) * live
    hs = dot(hot_rt, hidden).astype(BF16)
    hs_b[...] = hs
    for d in far_first(ny):
        push("hs", hs_b, hs_g.at[d - 1], at_y(d))
    hand_on("wn2", wn2_g)
    geo = t_dot(ge, hidden)
    wn2 = wn_ref[1]
    arrived("wout_c", wout_g.at[:, 1 - c])
    arrived("hs", hs_g)
    for d in far_first(ny):
        yd = pl.multiple_of(lax.rem(y + d, ny) * fs_w + c * fw2, fw2)
        push("rows", win_ref.at[:, pl.ds(yd, fw2)], rows_g.at[d - 1, c], at_y(d))
        push("wn1", wn_ref.at[0, pl.ds(yd, fw2)], wn1_g.at[d - 1, c], at_y(d))
    agg = dot(hs, wout)
    for d in range(1, ny):
        agg += dot(hs_g[d - 1], wout_g[d - 1].reshape(hs_w, d_feat))
    agg = agg.astype(BF16)

    arrived("wn2_c", wn2_g.at[:, 1 - c])
    arrived("nb", nb_g)

    def unit_grad(before, gradient, weight):
        npre = before + dot(agg, weight)
        nsg = sigmoid(npre)
        slope = nsg * (1.0 + npre * (1.0 - nsg))
        return npre * nsg, (gradient * slope).astype(BF16)

    nhid, npg = unit_grad(base_n, gn_w, wn2)
    nhid = nhid.astype(BF16)
    npgs = [npg]
    grad_agg = dot_t(npg, wn2)
    for d in range(1, ny):
        weight = wn2_g[d - 1].reshape(d_feat, hs_w)
        _, other = unit_grad(
            nb_g[d - 1, 1].astype(F32), nb_g[d - 1, 0].astype(F32), weight
        )
        npgs.append(other)
        grad_agg += dot_t(other, weight)
    grad_agg = grad_agg.astype(BF16)

    ni, eo, ei = 2 * d_feat // owners, d_feat // owners, 3 * d_feat // owners

    def owner(n):
        return n % 2, (n // 2) % nx, n // nxc

    def for_owners(blocks, sources, out):
        for n in range(owners):
            oc, ox, oz = owner(n)
            at, start = blocks.at[oc, ox, oz], 0
            for size, source in sources:
                if len(blocks.shape) == 5:
                    at[start : start + size] = source[n * size : (n + 1) * size]
                else:
                    for row in range(0, size, 4):
                        four = source[n * size + row : n * size + row + 4]
                        at[(start + row) // 4] = four
                start += size
        out[...] = blocks[...].astype(BF16)

    g4[...] = dot(gn_t[...], nhid)
    g2[0:d_feat] = dot(n_t[...], npg)
    g2[d_feat:] = t_dot(agg, npg)
    for_owners(ga_f, ((ni, g2), (eo, g4)), ha)
    push("core_a", ha.at[1 - c], ca, {"c": 1 - c})

    epg = ((ge_w + picked(hot_r[...], dot_t(grad_agg, wout))) * slope).astype(BF16)
    epg_b[...] = epg
    for d in far_first(ny):
        push("epg", epg_b, epg_g.at[d - 1], at_y(d))

    def add_core(phase, own, got, to, out, slots):
        arrived(phase, got)
        out[...] = (own[c].astype(F32) + got[...].astype(F32)).astype(BF16)
        for d in far_first(nx):
            xd = lax.rem(x + d, nx)
            push(to, out.at[xd], slots.at[d - 1], {"x": xd})

    def add_x(phase, own, got, to, out, slots):
        arrived(phase, got)
        total = own[x].astype(F32)
        for d in range(1, nx):
            total += got[d - 1].astype(F32)
        out[...] = total.astype(BF16)
        for d in far_first(nz):
            zd = lax.rem(z + d, nz)
            push(to, out.at[zd], slots.at[d - 1], {"z": zd})

    def add_z(phase, own, got):
        arrived(phase, got)
        total = own[z].astype(F32)
        for d in range(1, nz):
            total += got[d - 1].astype(F32)
        return total

    s_sum = dot(hot_st, epg)
    s_hot = s_sum.astype(BF16)
    h_hot = dot(hot_ht, epg).astype(BF16)
    r_hot = dot(hot_rt, epg).astype(BF16)
    g3[...] = geo + t_dot(grad_agg, hs)
    g1[0:d_feat] = dot(e_t[...], epg)
    g1[2 * d_feat :] = dot(n_t[...], r_hot)
    arrived("raw2", r2.at[pl.ds(1, nz - 1)])
    halo = r2[...].reshape(owners, d_feat)
    g1[d_feat : 2 * d_feat] = dot(n_t[...], s_hot) + t_dot(halo, h_hot)
    for_owners(gb_f, ((ei, g1), (eo, g3)), hb)
    push("core_b", hb.at[1 - c], cb, {"c": 1 - c})
    add_core("core_a", ha, ca, "x_a", xa, rxa)

    back_out[...] = dot(hot_pt, epg).reshape(owners, 1, hs_w)
    back_in[0] = back_out[0]
    add_core("core_b", hb, cb, "x_b", xb, rxb)
    for k, d in everyone:
        at = k * nz + d
        push("back", back_out.at[at], back_in.at[at], at_xc(k, -1) | at_z(d, -1))
    hand_on("rows", rows_g)
    hand_on("wn1", wn1_g)
    add_x("x_a", xa, rxa, "z_a", za, rza)

    mine = pl.ds(pl.multiple_of(y * fs_w, fs_w), fs_w)
    arrived("epg", epg_g)
    arrived("rows_c", rows_g.at[:, 1 - c])
    arrived("wn1_c", wn1_g.at[:, 1 - c])
    w_s = [win_ref[1, mine]]
    grad_e = ge_ref[:, mine].astype(F32) + dot_t(epg, win_ref[0, mine])
    grad_n = (
        gn_ref[:, mine].astype(F32)
        + dot_t(npg, wn_ref[0, mine])
        + dot_t(r_hot, win_ref[2, mine])
    )
    for d in range(1, ny):
        part = epg_g[d - 1]
        r_d = dot(hot_rt, part).astype(BF16)
        w_e, w_sender, w_r = (
            jnp.concatenate([rows_g[d - 1, 0, b], rows_g[d - 1, 1, b]], axis=0)
            for b in range(3)
        )
        w_s.append(w_sender)
        grad_e += dot_t(part, w_e)
        grad_n += dot_t(r_d, w_r) + dot_t(npgs[d], wn1_g[d - 1].reshape(fs_w, hs_w))
    o_wide[0:ed] = grad_e.astype(BF16)

    add_x("x_b", xb, rxb, "z_b", zb, rzb)

    arrived("back", back_in.at[pl.ds(1, owners - 1)])
    high, low = two_parts(back_in[...].reshape(owners, hs_w))
    sums = (s_sum + dot(sl_perm, high) + dot(sl_perm, low)).astype(BF16)
    sums_b[...] = sums
    for d in far_first(ny):
        push("sums", sums_b, sums_g.at[d - 1], at_y(d))
    total_a = add_z("z_a", za, rza)
    for i in range(total_a.shape[0]):
        o_rows[4 * i : 4 * i + 4] = total_a[i]
    grad_n += dot_t(sums, w_s[0])
    arrived("sums", sums_g)
    for d in range(1, ny):
        grad_n += dot_t(sums_g[d - 1], w_s[d])
    o_wide[ed:] = grad_n.astype(BF16)
    left("halo", p_in.at[pl.ds(1, owners - 1)])
    left("raw1", out1.at[pl.ds(1, nxc - 1)])
    left("raw2", out2.at[pl.ds(1, nz - 1)])
    for phase, buf in (
        ("wout", wout_g),
        ("wn2", wn2_g),
        ("rows", rows_g),
        ("wn1", wn1_g),
    ):
        left(phase, buf.at[:, c])
        left(phase + "_c", buf.at[:, c])
    left("nb", nb_g)
    left("hs", hs_g)
    left("epg", epg_g)
    left("core_a", ca)
    left("core_b", cb)
    left("x_a", rxa)
    left("x_b", rxb)
    left("z_a", rza)
    left("z_b", rzb)
    left("back", back_in.at[pl.ds(1, owners - 1)])
    left("sums", sums_g)

    total_b = add_z("z_b", zb, rzb)
    o_rows[ni + eo :] = total_b


def hand_out(wide, rows, o_nodes, o_edges, o_ei, o_eo, o_ni, o_no):
    ed, ni, eo, ei = o_edges.shape[0], o_ni.shape[0], o_eo.shape[0], o_ei.shape[0]
    second = rows.shape[0] - ei - eo
    o_edges[...] = wide[0:ed]
    o_nodes[...] = wide[ed:]
    o_ni[...] = rows[0:ni]
    o_no[...] = rows[ni : ni + eo]
    o_ei[...] = rows[second : second + ei]
    o_eo[...] = rows[second + ei :]


def body(nz, nx, ny, nodes, edges, gn, ge, win, be, wout, wn, bn, wno, snd, rcv, vc, sl):
    nd, d = nodes.shape
    ed = edges.shape[0]
    hw = wout.shape[0]
    fw = d // ny
    nxc = 2 * nx
    owners = nz * nxc
    ni, eo, ei = 2 * d // owners, d // owners, 3 * d // owners
    ra = (ni + eo) // 4
    rb = ei + eo
    vm = pltpu.VMEM
    phases = len(PHASES)
    v_spec = pl.BlockSpec(memory_space=pltpu.VMEM)
    wide, rows = pl.pallas_call(
        functools.partial(kernel, nz, nx, ny),
        out_shape=(vm((ed + nd, fw), BF16), vm((4 * ra + rb, hw), F32)),
        in_specs=[pl.BlockSpec(memory_space=pl.ANY)] * 14,
        out_specs=(v_spec,) * 2,
        scratch_shapes=[
            vm((1, owners), jnp.int32),
            vm((ed,), jnp.int32),
            vm((ed,), jnp.int32),
            pltpu.SMEM((vc.shape[0],), jnp.int32),
            vm((nd, d), BF16),
            vm((ed, d), BF16),
            vm((nd, d), BF16),
            vm((ed, d), BF16),
            vm((3, d, hw), BF16),
            vm((1, hw), F32),
            vm((hw, d), BF16),
            vm((2, d, hw), BF16),
            vm((1, hw), F32),
            vm((hw, d), BF16),
            pltpu.SemaphoreType.DMA((14,)),
            vm((owners, 1, hw), F32),
            vm((owners, 1, hw), F32),
            vm((nxc, nz, d), BF16),
            vm((nxc, nz, d), BF16),
            vm((nz, nxc, d), BF16),
            vm((nz, nxc, d), BF16),
            vm((ny - 1, 2, hw // 2, d), BF16),
            vm((ny - 1, 2, d // 2, hw), BF16),
            vm((ny - 1, 2, 3, fw // 2, hw), BF16),
            vm((ny - 1, 2, fw // 2, hw), BF16),
            vm((2, nd, hw), BF16),
            vm((ny - 1, 2, nd, hw), BF16),
            vm((nd, hw), BF16),
            vm((ny - 1, nd, hw), BF16),
            vm((ed, hw), BF16),
            vm((ny - 1, ed, hw), BF16),
            vm((2, nx, nz, ra, 4, hw), F32),
            vm((2, nx, nz, rb, hw), F32),
            vm((3 * d, hw), F32),
            vm((2 * d, hw), F32),
            vm((d, hw), F32),
            vm((d, hw), F32),
            vm((2, nx, nz, ra, 4, hw), BF16),
            vm((2, nx, nz, rb, hw), BF16),
            vm((nx, nz, ra, 4, hw), BF16),
            vm((nx, nz, rb, hw), BF16),
            vm((nx, nz, ra, 4, hw), BF16),
            vm((nx, nz, rb, hw), BF16),
            vm((nx - 1, nz, ra, 4, hw), BF16),
            vm((nx - 1, nz, rb, hw), BF16),
            vm((nz, ra, 4, hw), BF16),
            vm((nz, rb, hw), BF16),
            vm((nz - 1, ra, 4, hw), BF16),
            vm((nz - 1, rb, hw), BF16),
            vm((owners, 1, hw), F32),
            vm((owners, 1, hw), F32),
            vm((nd, hw), BF16),
            vm((ny - 1, nd, hw), BF16),
            vm((ed, owners), BF16),
            vm((ed, nd), BF16),
            vm((d, nd), BF16),
            vm((d, nd), BF16),
            vm((d, ed), BF16),
            pltpu.SemaphoreType.DMA((phases,)),
            pltpu.SemaphoreType.DMA((phases,)),
        ],
        compiler_params=pltpu.CompilerParams(collective_id=0, has_side_effects=True),
    )(
        sl.reshape(1, owners),
        snd,
        rcv,
        vc,
        nodes,
        edges,
        gn,
        ge,
        win.reshape(3, d, hw),
        be.reshape(1, hw),
        wout,
        wn.reshape(2, d, hw),
        bn.reshape(1, hw),
        wno,
    )
    g_nodes, g_edges, g_ei, g_eo, g_ni, g_no = pl.pallas_call(
        hand_out,
        out_shape=(
            jax.ShapeDtypeStruct((nd, fw), BF16),
            jax.ShapeDtypeStruct((ed, fw), BF16),
            jax.ShapeDtypeStruct((ei, hw), F32),
            jax.ShapeDtypeStruct((eo, hw), F32),
            jax.ShapeDtypeStruct((ni, hw), F32),
            jax.ShapeDtypeStruct((eo, hw), F32),
        ),
        in_specs=[v_spec] * 2,
        out_specs=(v_spec,) * 6,
    )(*(pltpu.with_memory_space_constraint(v, pltpu.VMEM) for v in (wide, rows)))
    return g_nodes, g_edges, g_ei, g_eo.T, g_ni, g_no.T


def solution(mesh):
    ny = mesh.shape["chan"]
    nx = 4 if mesh.shape["node"] == 128 else 2
    nz = mesh.shape["node"] // (2 * nx)
    split = Mesh(mesh.devices.reshape(nz, nx, 2, ny), ("z", "x", "c", "y"))
    in_specs = (
        P(NODE, None),
        P(NODE, None),
        P(NODE, None),
        P(NODE, None),
        P(None, "y"),
        P("y"),
        P("y", None),
        P(None, "y"),
        P("y"),
        P("y", None),
        P(NODE),
        P(NODE),
        P(NODE),
        P(NODE, None),
    )
    out_specs = (
        P(NODE, "y"),
        P(NODE, "y"),
        P(NODE, "y"),
        P("y", NODE),
        P(NODE, "y"),
        P("y", NODE),
    )
    return jax.shard_map(
        functools.partial(body, nz, nx, ny),
        mesh=split,
        in_specs=in_specs,
        out_specs=out_specs,
        check_vma=False,
    )
```

```python
import functools

import jax
import jax.numpy as jnp
from jax import lax
from jax.experimental import pallas as pl
from jax.experimental.pallas import tpu as pltpu
from jax.sharding import Mesh
from jax.sharding import PartitionSpec as P

NODE = ("z", "x", "c")
MESH = pl.DeviceIdType.MESH
F32 = jnp.float32
BF16 = jnp.bfloat16


def dot(a, b):
    return jnp.dot(a, b, preferred_element_type=F32)


def dot_t(a, b):
    return lax.dot_general(a, b, (((1,), (1,)), ((), ())), preferred_element_type=F32)


def t_dot(a, b):
    return lax.dot_general(a, b, (((0,), (0,)), ((), ())), preferred_element_type=F32)


def iota(shape, dim):
    return lax.broadcasted_iota(jnp.int32, shape, dim)


def hot(cond):
    return jnp.where(cond, 1.0, 0.0).astype(BF16)


def two_parts(v):
    high = v.astype(BF16)
    return high, (v - high.astype(F32)).astype(BF16)


def sigmoid(v):
    return 1.0 / (1.0 + jnp.exp(-v))


PHASES = (
    "halo",
    "raw1",
    "raw2",
    "wout",
    "wout_c",
    "wn2",
    "wn2_c",
    "nb",
    "rows",
    "rows_c",
    "wn1",
    "wn1_c",
    "hs",
    "epg",
    "core_a",
    "core_b",
    "x_a",
    "x_b",
    "z_a",
    "z_b",
    "back",
    "sums",
)


def kernel(
    nz,
    nx,
    ny,
    sl_in,
    snd_in,
    rcv_in,
    vc_in,
    n_in,
    e_in,
    gn_in,
    ge_in,
    win_in,
    be_in,
    wout_in,
    wn_in,
    bn_in,
    wno_in,
    o_wide,
    o_rows,
    sl_ref,
    snd_ref,
    rcv_ref,
    vc_ref,
    n_ref,
    e_ref,
    gn_ref,
    ge_ref,
    win_ref,
    be_ref,
    wout_ref,
    wn_ref,
    bn_ref,
    wno_ref,
    load,
    p_out,
    p_in,
    out1,
    r1,
    out2,
    r2,
    wout_g,
    wn2_g,
    rows_g,
    wn1_g,
    nb_b,
    nb_g,
    hs_b,
    hs_g,
    epg_b,
    epg_g,
    gb_f,
    g1,
    g3,
    ha,
    hb,
    ca,
    cb,
    xa,
    xb,
    rxa,
    rxb,
    za,
    zb,
    rza,
    rzb,
    back_out,
    back_in,
    sums_b,
    sums_g,
    hot_p,
    hot_r,
    n_t,
    gn_t,
    e_t,
    wout_f,
    wn2_f,
    both,
    send,
    recv,
):
    z, x, c, y = (lax.axis_index(a) for a in ("z", "x", "c", "y"))
    nxc = 2 * nx
    owners = nz * nxc
    nd, d_feat = n_ref.shape
    ed = e_ref.shape[0]
    hs_w = wout_ref.shape[0]
    fs_w = d_feat // ny
    block = ed // vc_ref.shape[0]

    def by(**kw):
        return kw

    def at_xc(k, sign=1):
        place = {}
        if k // 2:
            place["x"] = lax.rem(x + nx + sign * (k // 2), nx)
        if k % 2:
            place["c"] = 1 - c
        return place

    def at_z(d, sign=1):
        return {"z": lax.rem(z + nz + sign * d, nz)} if d else {}

    def at_y(d):
        return {"y": lax.rem(y + d, ny)}

    def hops(k, d):
        return min(d, nz - d) + min(k // 2, nx - k // 2)

    def far_first(n):
        return sorted(range(1, n), key=lambda d: -min(d, n - d))

    everyone = [(k, d) for k in range(nxc) for d in range(nz) if k or d]
    everyone.sort(key=lambda kd: -hops(*kd))

    sources = (sl_in, n_in, win_in, wout_in, wn_in, e_in, snd_in, rcv_in, vc_in, be_in, bn_in, ge_in, gn_in, wno_in)
    places = (sl_ref, n_ref, win_ref, wout_ref, wn_ref, e_ref, snd_ref, rcv_ref, vc_ref, be_ref, bn_ref, ge_ref, gn_ref, wno_ref)
    loads = [pltpu.make_async_copy(a, b, load.at[i]) for i, (a, b) in enumerate(zip(sources, places))]

    barrier = pltpu.get_barrier_semaphore()
    peers = [at_xc(k) | at_z(d) for k, d in everyone] + [at_y(d) for d in range(1, ny)]
    for peer in peers:
        pl.semaphore_signal(barrier, inc=1, device_id=peer, device_id_type=MESH)
    for copy in loads:
        copy.start()

    def push(phase, src, dst, peer):
        pltpu.make_async_remote_copy(
            src_ref=src,
            dst_ref=dst,
            send_sem=send.at[PHASES.index(phase)],
            recv_sem=recv.at[PHASES.index(phase)],
            device_id=peer,
            device_id_type=MESH,
        ).start()

    def arrived(phase, ref):
        with jax.named_scope(f"wait_{phase}"):
            pltpu.make_async_copy(ref, ref, recv.at[PHASES.index(phase)]).wait()

    def left(phase, ref):
        pltpu.make_async_copy(ref, ref, send.at[PHASES.index(phase)]).wait()

    with jax.named_scope("load0"):
        for copy in loads[:2]:
            copy.wait()
    nodes = n_ref[...]
    r_q = iota((owners, owners), 1)
    k_of, dz_of = r_q // nz, r_q % nz
    q_of = (
        ((z + dz_of) & (nz - 1)) * nxc
        + ((x + (k_of >> 1)) & (nx - 1)) * 2
        + (c ^ (k_of & 1))
    )
    perm_q = hot(iota((owners, owners), 0) == q_of)
    sl_hot = hot(iota((nd, owners), 0) == sl_ref[...])
    sl_perm = dot(sl_hot, perm_q).astype(BF16)
    rows_out = t_dot(sl_perm, nodes).astype(BF16)
    for copy in loads[2:3]:
        copy.wait()
    p_out[...] = dot(rows_out, win_ref[1]).reshape(owners, 1, hs_w)
    p_in[0] = p_out[0]
    for k in range(nxc):
        out1[k] = rows_out[k * nz : (k + 1) * nz]
    r1[0] = rows_out[0:nz]

    with jax.named_scope("entry"):
        pl.semaphore_wait(barrier, len(peers))

    for k, d in everyone:
        push("halo", p_out.at[k * nz + d], p_in.at[k * nz + d], at_xc(k) | at_z(d))
    for k in range(1, nxc):
        push("raw1", out1.at[k], r1.at[k], at_xc(k))

    hw2, dw2, fw2 = hs_w // 2, d_feat // 2, fs_w // 2
    for copy in loads[3:5]:
        copy.wait()
    for d in far_first(ny):
        push("wout", wout_ref.at[pl.ds(c * hw2, hw2)], wout_g.at[d - 1, c], at_y(d))
    for d in far_first(ny):
        push("wn2", wn_ref.at[1, pl.ds(c * dw2, dw2)], wn2_g.at[d - 1, c], at_y(d))

    def hand_on(phase, buf):
        arrived(phase, buf.at[:, c])
        for d in far_first(ny):
            push(phase + "_c", buf.at[d - 1, c], buf.at[d - 1, c], {"c": 1 - c})

    for copy in loads[5:]:
        copy.wait()
    gn = gn_ref[...]
    gn_w = dot_t(gn, wno_ref[...])
    base_n = dot(nodes, wn_ref[0]) + bn_ref[...]
    nb_b[0] = gn_w.astype(BF16)
    nb_b[1] = base_n.astype(BF16)
    for d in far_first(ny):
        push("nb", nb_b, nb_g.at[d - 1], at_y(d))

    snd, rcv = snd_ref[...].reshape(1, ed), rcv_ref[...].reshape(1, ed)

    def remote(k, dz):
        owner_of = (
            ((z - dz) & (nz - 1)) * nxc
            + ((x - (k >> 1)) & (nx - 1)) * 2
            + (c ^ (k & 1))
        )
        return hot(owner_of + nd == snd)

    t_e = iota((owners, ed), 0)
    hot_pt = remote(t_e // nz, t_e % nz)
    hot_ht = remote(t_e % nxc, t_e // nxc)
    hot_st = hot(iota((nd, ed), 0) == snd)
    hot_rt = hot(iota((nd, ed), 0) == rcv)

    def picked(onehot, table):
        high, low = two_parts(table)
        return dot(onehot, high) + dot(onehot, low)

    hot_p[...] = jnp.transpose(hot_pt)
    hot_r[...] = jnp.transpose(hot_rt)

    live = jnp.concatenate(
        [
            jnp.where(iota((block, hs_w), 0) < vc_ref[b], 1.0, 0.0)
            for b in range(ed // block)
        ],
        axis=0,
    )
    edges = e_ref[...]
    base = (
        dot(edges, win_ref[0])
        + be_ref[...]
        + picked(jnp.transpose(hot_st), dot(nodes, win_ref[1]))
        + picked(hot_r[...], dot(nodes, win_ref[2]))
    )
    ge = ge_ref[...]
    wout = wout_ref[...]
    ge_w = dot_t(ge, wout)

    n_t[...] = jnp.transpose(nodes)
    gn_t[...] = jnp.transpose(gn)
    e_t[...] = jnp.transpose(edges)

    t_i = iota((owners, owners), 0)
    stage = hot(iota((owners, owners), 1) == (t_i % nxc) * nz + t_i // nxc)
    arrived("raw1", r1.at[pl.ds(1, nxc - 1)])
    second = dot(stage, r1[...].reshape(owners, d_feat)).astype(BF16)
    for d in range(nz):
        out2[d] = second[d * nxc : (d + 1) * nxc]
    r2[0] = second[0:nxc]
    for d in far_first(nz):
        push("raw2", out2.at[d], r2.at[d], at_z(d))
    hand_on("wout", wout_g)

    arrived("halo", p_in.at[pl.ds(1, owners - 1)])
    pre = base + picked(hot_p[...], p_in[...].reshape(owners, hs_w))
    sg = sigmoid(pre)
    hidden = (pre * sg * live).astype(BF16)
    slope = sg * (1.0 + pre * (1.0 - sg)) * live
    hs = dot(hot_rt, hidden).astype(BF16)
    hs_b[...] = hs
    for d in far_first(ny):
        push("hs", hs_b, hs_g.at[d - 1], at_y(d))
    hand_on("wn2", wn2_g)
    geo = t_dot(ge, hidden)
    arrived("wout_c", wout_g.at[:, 1 - c])
    arrived("wn2_c", wn2_g.at[:, 1 - c])
    arrived("nb", nb_g)
    wout_f[0:hs_w] = wout
    wn2_f[:, 0:hs_w] = wn_ref[1]
    for d in range(1, ny):
        share = slice(d * hs_w, (d + 1) * hs_w)
        wout_f[share] = wout_g[d - 1].reshape(hs_w, d_feat)
        wn2_f[:, share] = wn2_g[d - 1].reshape(d_feat, hs_w)
    both[...] = dot(wout_f[...], wn2_f[...]).astype(BF16)
    before = jnp.concatenate(
        [base_n] + [nb_g[d - 1, 1].astype(F32) for d in range(1, ny)], axis=1
    )
    gradient = jnp.concatenate(
        [gn_w] + [nb_g[d - 1, 0].astype(F32) for d in range(1, ny)], axis=1
    )

    arrived("hs", hs_g)
    for d in far_first(ny):
        yd = pl.multiple_of(lax.rem(y + d, ny) * fs_w + c * fw2, fw2)
        push("rows", win_ref.at[:, pl.ds(yd, fw2)], rows_g.at[d - 1, c], at_y(d))
        push("wn1", wn_ref.at[0, pl.ds(yd, fw2)], wn1_g.at[d - 1, c], at_y(d))
    hs_f = jnp.concatenate([hs] + [hs_g[d - 1] for d in range(1, ny)], axis=1)
    npre = before + dot(hs_f, both[...])
    nsg = sigmoid(npre)
    nhid = (npre * nsg)[:, 0:hs_w].astype(BF16)
    npg_f = (gradient * (nsg * (1.0 + npre * (1.0 - nsg)))).astype(BF16)
    npgs = [npg_f[:, d * hs_w : (d + 1) * hs_w] for d in range(ny)]
    npg = npgs[0]
    agg = dot(hs_f, wout_f[...]).astype(BF16)

    ni, eo, ei = 2 * d_feat // owners, d_feat // owners, 3 * d_feat // owners

    def owner(n):
        return n % 2, (n // 2) % nx, n // nxc

    def in_fours(start, size, value):
        fours = value.reshape(-1, 4, hs_w).astype(BF16)
        for n in range(owners):
            oc, ox, oz = owner(n)
            for i in range(size // 4):
                ha[oc, ox, oz, start // 4 + i] = fours[n * size // 4 + i]

    in_fours(
        0, ni, jnp.concatenate([dot(n_t[...], npg), t_dot(agg, npg)], axis=0)
    )
    in_fours(ni, eo, dot(gn_t[...], nhid))
    push("core_a", ha.at[1 - c], ca, {"c": 1 - c})

    epg = ((ge_w + picked(hot_r[...], dot_t(npg_f, both[0:hs_w]))) * slope).astype(BF16)
    epg_b[...] = epg
    for d in far_first(ny):
        push("epg", epg_b, epg_g.at[d - 1], at_y(d))

    def add_core(phase, own, got, to, out, slots):
        arrived(phase, got)
        out[...] = (own[c].astype(F32) + got[...].astype(F32)).astype(BF16)
        for d in far_first(nx):
            xd = lax.rem(x + d, nx)
            push(to, out.at[xd], slots.at[d - 1], {"x": xd})

    def add_x(phase, own, got, to, out, slots):
        arrived(phase, got)
        total = own[x].astype(F32)
        for d in range(1, nx):
            total += got[d - 1].astype(F32)
        out[...] = total.astype(BF16)
        for d in far_first(nz):
            zd = lax.rem(z + d, nz)
            push(to, out.at[zd], slots.at[d - 1], {"z": zd})

    def add_z(phase, own, got):
        arrived(phase, got)
        total = own[z].astype(F32)
        for d in range(1, nz):
            total += got[d - 1].astype(F32)
        return total

    grad_agg = dot_t(npg_f, wn2_f[...]).astype(BF16)
    s_sum = dot(hot_st, epg)
    s_hot = s_sum.astype(BF16)
    h_hot = dot(hot_ht, epg).astype(BF16)
    r_hot = dot(hot_rt, epg).astype(BF16)
    g3[...] = geo + t_dot(grad_agg, hs)
    g1[0:d_feat] = dot(e_t[...], epg)
    g1[2 * d_feat :] = dot(n_t[...], r_hot)
    arrived("raw2", r2.at[pl.ds(1, nz - 1)])
    halo = r2[...].reshape(owners, d_feat)
    g1[d_feat : 2 * d_feat] = dot(n_t[...], s_hot) + t_dot(halo, h_hot)
    for n in range(owners):
        oc, ox, oz = owner(n)
        gb_f[oc, ox, oz, 0:ei] = g1[n * ei : (n + 1) * ei]
        gb_f[oc, ox, oz, ei:] = g3[n * eo : (n + 1) * eo]
    hb[...] = gb_f[...].astype(BF16)
    push("core_b", hb.at[1 - c], cb, {"c": 1 - c})
    add_core("core_a", ha, ca, "x_a", xa, rxa)

    back_out[...] = dot(hot_pt, epg).reshape(owners, 1, hs_w)
    back_in[0] = back_out[0]
    add_core("core_b", hb, cb, "x_b", xb, rxb)
    for k, d in everyone:
        at = k * nz + d
        push("back", back_out.at[at], back_in.at[at], at_xc(k, -1) | at_z(d, -1))
    hand_on("rows", rows_g)
    hand_on("wn1", wn1_g)
    add_x("x_a", xa, rxa, "z_a", za, rza)

    mine = pl.ds(pl.multiple_of(y * fs_w, fs_w), fs_w)
    arrived("epg", epg_g)
    arrived("rows_c", rows_g.at[:, 1 - c])
    arrived("wn1_c", wn1_g.at[:, 1 - c])
    w_s = [win_ref[1, mine]]
    grad_e = ge_ref[:, mine].astype(F32) + dot_t(epg, win_ref[0, mine])
    grad_n = (
        gn_ref[:, mine].astype(F32)
        + dot_t(npg, wn_ref[0, mine])
        + dot_t(r_hot, win_ref[2, mine])
    )
    for d in range(1, ny):
        part = epg_g[d - 1]
        r_d = dot(hot_rt, part).astype(BF16)
        w_e, w_sender, w_r = (
            jnp.concatenate([rows_g[d - 1, 0, b], rows_g[d - 1, 1, b]], axis=0)
            for b in range(3)
        )
        w_s.append(w_sender)
        grad_e += dot_t(part, w_e)
        grad_n += dot_t(r_d, w_r) + dot_t(npgs[d], wn1_g[d - 1].reshape(fs_w, hs_w))
    o_wide[0:ed] = grad_e.astype(BF16)

    add_x("x_b", xb, rxb, "z_b", zb, rzb)

    arrived("back", back_in.at[pl.ds(1, owners - 1)])
    high, low = two_parts(back_in[...].reshape(owners, hs_w))
    sums = (s_sum + dot(sl_perm, high) + dot(sl_perm, low)).astype(BF16)
    sums_b[...] = sums
    for d in far_first(ny):
        push("sums", sums_b, sums_g.at[d - 1], at_y(d))
    total_a = add_z("z_a", za, rza)
    for i in range(total_a.shape[0]):
        o_rows[4 * i : 4 * i + 4] = total_a[i]
    grad_n += dot_t(sums, w_s[0])
    arrived("sums", sums_g)
    for d in range(1, ny):
        grad_n += dot_t(sums_g[d - 1], w_s[d])
    o_wide[ed:] = grad_n.astype(BF16)
    left("halo", p_in.at[pl.ds(1, owners - 1)])
    left("raw1", out1.at[pl.ds(1, nxc - 1)])
    left("raw2", out2.at[pl.ds(1, nz - 1)])
    for phase, buf in (
        ("wout", wout_g),
        ("wn2", wn2_g),
        ("rows", rows_g),
        ("wn1", wn1_g),
    ):
        left(phase, buf.at[:, c])
        left(phase + "_c", buf.at[:, c])
    left("nb", nb_g)
    left("hs", hs_g)
    left("epg", epg_g)
    left("core_a", ca)
    left("core_b", cb)
    left("x_a", rxa)
    left("x_b", rxb)
    left("z_a", rza)
    left("z_b", rzb)
    left("back", back_in.at[pl.ds(1, owners - 1)])
    left("sums", sums_g)

    total_b = add_z("z_b", zb, rzb)
    o_rows[ni + eo :] = total_b


def hand_out(wide, rows, o_nodes, o_edges, o_ei, o_eo, o_ni, o_no):
    ed, ni, eo, ei = o_edges.shape[0], o_ni.shape[0], o_eo.shape[0], o_ei.shape[0]
    second = rows.shape[0] - ei - eo
    o_edges[...] = wide[0:ed]
    o_nodes[...] = wide[ed:]
    o_ni[...] = rows[0:ni]
    o_no[...] = rows[ni : ni + eo]
    o_ei[...] = rows[second : second + ei]
    o_eo[...] = rows[second + ei :]


def body(nz, nx, ny, nodes, edges, gn, ge, win, be, wout, wn, bn, wno, snd, rcv, vc, sl):
    nd, d = nodes.shape
    ed = edges.shape[0]
    hw = wout.shape[0]
    fw = d // ny
    nxc = 2 * nx
    owners = nz * nxc
    ni, eo, ei = 2 * d // owners, d // owners, 3 * d // owners
    ra = (ni + eo) // 4
    rb = ei + eo
    vm = pltpu.VMEM
    phases = len(PHASES)
    v_spec = pl.BlockSpec(memory_space=pltpu.VMEM)
    wide, rows = pl.pallas_call(
        functools.partial(kernel, nz, nx, ny),
        out_shape=(vm((ed + nd, fw), BF16), vm((4 * ra + rb, hw), F32)),
        in_specs=[pl.BlockSpec(memory_space=pl.ANY)] * 14,
        out_specs=(v_spec,) * 2,
        scratch_shapes=[
            vm((1, owners), jnp.int32),
            vm((ed,), jnp.int32),
            vm((ed,), jnp.int32),
            pltpu.SMEM((vc.shape[0],), jnp.int32),
            vm((nd, d), BF16),
            vm((ed, d), BF16),
            vm((nd, d), BF16),
            vm((ed, d), BF16),
            vm((3, d, hw), BF16),
            vm((1, hw), F32),
            vm((hw, d), BF16),
            vm((2, d, hw), BF16),
            vm((1, hw), F32),
            vm((hw, d), BF16),
            pltpu.SemaphoreType.DMA((14,)),
            vm((owners, 1, hw), F32),
            vm((owners, 1, hw), F32),
            vm((nxc, nz, d), BF16),
            vm((nxc, nz, d), BF16),
            vm((nz, nxc, d), BF16),
            vm((nz, nxc, d), BF16),
            vm((ny - 1, 2, hw // 2, d), BF16),
            vm((ny - 1, 2, d // 2, hw), BF16),
            vm((ny - 1, 2, 3, fw // 2, hw), BF16),
            vm((ny - 1, 2, fw // 2, hw), BF16),
            vm((2, nd, hw), BF16),
            vm((ny - 1, 2, nd, hw), BF16),
            vm((nd, hw), BF16),
            vm((ny - 1, nd, hw), BF16),
            vm((ed, hw), BF16),
            vm((ny - 1, ed, hw), BF16),
            vm((2, nx, nz, rb, hw), F32),
            vm((3 * d, hw), F32),
            vm((d, hw), F32),
            vm((2, nx, nz, ra, 4, hw), BF16),
            vm((2, nx, nz, rb, hw), BF16),
            vm((nx, nz, ra, 4, hw), BF16),
            vm((nx, nz, rb, hw), BF16),
            vm((nx, nz, ra, 4, hw), BF16),
            vm((nx, nz, rb, hw), BF16),
            vm((nx - 1, nz, ra, 4, hw), BF16),
            vm((nx - 1, nz, rb, hw), BF16),
            vm((nz, ra, 4, hw), BF16),
            vm((nz, rb, hw), BF16),
            vm((nz - 1, ra, 4, hw), BF16),
            vm((nz - 1, rb, hw), BF16),
            vm((owners, 1, hw), F32),
            vm((owners, 1, hw), F32),
            vm((nd, hw), BF16),
            vm((ny - 1, nd, hw), BF16),
            vm((ed, owners), BF16),
            vm((ed, nd), BF16),
            vm((d, nd), BF16),
            vm((d, nd), BF16),
            vm((d, ed), BF16),
            vm((ny * hw, d), BF16),
            vm((d, ny * hw), BF16),
            vm((ny * hw, ny * hw), BF16),
            pltpu.SemaphoreType.DMA((phases,)),
            pltpu.SemaphoreType.DMA((phases,)),
        ],
        compiler_params=pltpu.CompilerParams(collective_id=0, has_side_effects=True),
    )(
        sl.reshape(1, owners),
        snd,
        rcv,
        vc,
        nodes,
        edges,
        gn,
        ge,
        win.reshape(3, d, hw),
        be.reshape(1, hw),
        wout,
        wn.reshape(2, d, hw),
        bn.reshape(1, hw),
        wno,
    )
    g_nodes, g_edges, g_ei, g_eo, g_ni, g_no = pl.pallas_call(
        hand_out,
        out_shape=(
            jax.ShapeDtypeStruct((nd, fw), BF16),
            jax.ShapeDtypeStruct((ed, fw), BF16),
            jax.ShapeDtypeStruct((ei, hw), F32),
            jax.ShapeDtypeStruct((eo, hw), F32),
            jax.ShapeDtypeStruct((ni, hw), F32),
            jax.ShapeDtypeStruct((eo, hw), F32),
        ),
        in_specs=[v_spec] * 2,
        out_specs=(v_spec,) * 6,
    )(*(pltpu.with_memory_space_constraint(v, pltpu.VMEM) for v in (wide, rows)))
    return g_nodes, g_edges, g_ei, g_eo.T, g_ni, g_no.T


def solution(mesh):
    ny = mesh.shape["chan"]
    nx = 4 if mesh.shape["node"] == 128 else 2
    nz = mesh.shape["node"] // (2 * nx)
    split = Mesh(mesh.devices.reshape(nz, nx, 2, ny), ("z", "x", "c", "y"))
    in_specs = (
        P(NODE, None),
        P(NODE, None),
        P(NODE, None),
        P(NODE, None),
        P(None, "y"),
        P("y"),
        P("y", None),
        P(None, "y"),
        P("y"),
        P("y", None),
        P(NODE),
        P(NODE),
        P(NODE),
        P(NODE, None),
    )
    out_specs = (
        P(NODE, "y"),
        P(NODE, "y"),
        P(NODE, "y"),
        P("y", NODE),
        P(NODE, "y"),
        P("y", NODE),
    )
    return jax.shard_map(
        functools.partial(body, nz, nx, ny),
        mesh=split,
        in_specs=in_specs,
        out_specs=out_specs,
        check_vma=False,
    )
```

```python
import functools

import jax
import jax.numpy as jnp
from jax import lax
from jax.experimental import pallas as pl
from jax.experimental.pallas import tpu as pltpu
from jax.sharding import Mesh
from jax.sharding import PartitionSpec as P

NODE = ("z", "x", "c")
MESH = pl.DeviceIdType.MESH
F32 = jnp.float32
BF16 = jnp.bfloat16


def dot(a, b):
    return jnp.dot(a, b, preferred_element_type=F32)


def dot_t(a, b):
    return lax.dot_general(a, b, (((1,), (1,)), ((), ())), preferred_element_type=F32)


def t_dot(a, b):
    return lax.dot_general(a, b, (((0,), (0,)), ((), ())), preferred_element_type=F32)


def iota(shape, dim):
    return lax.broadcasted_iota(jnp.int32, shape, dim)


def hot(cond):
    return jnp.where(cond, 1.0, 0.0).astype(BF16)


def two_parts(v):
    high = v.astype(BF16)
    return high, (v - high.astype(F32)).astype(BF16)


def sigmoid(v):
    return 1.0 / (1.0 + jnp.exp(-v))


PHASES = (
    "halo",
    "raw1",
    "raw2",
    "wout",
    "wout_c",
    "wn2",
    "wn2_c",
    "nb",
    "rows",
    "rows_c",
    "wn1",
    "wn1_c",
    "hs",
    "epg",
    "core_a",
    "core_b",
    "x_a",
    "x_b",
    "z_a",
    "z_b",
    "back",
    "sums",
)


def kernel(
    nz,
    nx,
    ny,
    sl_in,
    snd_in,
    rcv_in,
    vc_in,
    n_in,
    e_in,
    gn_in,
    ge_in,
    win_in,
    be_in,
    wout_in,
    wn_in,
    bn_in,
    wno_in,
    o_wide,
    o_rows,
    sl_ref,
    snd_ref,
    rcv_ref,
    vc_ref,
    n_ref,
    e_ref,
    gn_ref,
    ge_ref,
    win_ref,
    be_ref,
    wout_ref,
    wn_ref,
    bn_ref,
    wno_ref,
    load,
    p_out,
    p_in,
    out1,
    r1,
    out2,
    r2,
    wout_g,
    wn2_g,
    rows_g,
    wn1_g,
    nb_b,
    nb_g,
    hs_b,
    hs_g,
    epg_b,
    epg_g,
    gb_f,
    g1,
    g3,
    ha,
    hb,
    ca,
    cb,
    xa,
    xb,
    rxa,
    rxb,
    za,
    zb,
    rza,
    rzb,
    back_out,
    back_in,
    sums_b,
    sums_g,
    hot_p,
    hot_r,
    n_t,
    gn_t,
    e_t,
    wout_f,
    wn2_f,
    both,
    send,
    recv,
):
    z, x, c, y = (lax.axis_index(a) for a in ("z", "x", "c", "y"))
    nxc = 2 * nx
    owners = nz * nxc
    nd, d_feat = n_ref.shape
    ed = e_ref.shape[0]
    hs_w = wout_ref.shape[0]
    fs_w = d_feat // ny
    block = ed // vc_ref.shape[0]

    def by(**kw):
        return kw

    def at_xc(k, sign=1):
        place = {}
        if k // 2:
            place["x"] = lax.rem(x + nx + sign * (k // 2), nx)
        if k % 2:
            place["c"] = 1 - c
        return place

    def at_z(d, sign=1):
        return {"z": lax.rem(z + nz + sign * d, nz)} if d else {}

    def at_y(d):
        return {"y": lax.rem(y + d, ny)}

    def hops(k, d):
        return min(d, nz - d) + min(k // 2, nx - k // 2)

    def far_first(n):
        return sorted(range(1, n), key=lambda d: -min(d, n - d))

    everyone = [(k, d) for k in range(nxc) for d in range(nz) if k or d]
    everyone.sort(key=lambda kd: -hops(*kd))

    sources = (sl_in, n_in, win_in, wout_in, wn_in, e_in, snd_in, rcv_in, vc_in, be_in, bn_in, ge_in, gn_in, wno_in)
    places = (sl_ref, n_ref, win_ref, wout_ref, wn_ref, e_ref, snd_ref, rcv_ref, vc_ref, be_ref, bn_ref, ge_ref, gn_ref, wno_ref)
    loads = [pltpu.make_async_copy(a, b, load.at[i]) for i, (a, b) in enumerate(zip(sources, places))]

    barrier = pltpu.get_barrier_semaphore()
    peers = [at_xc(k) | at_z(d) for k, d in everyone] + [at_y(d) for d in range(1, ny)]
    for peer in peers:
        pl.semaphore_signal(barrier, inc=1, device_id=peer, device_id_type=MESH)
    for copy in loads:
        copy.start()

    def push(phase, src, dst, peer):
        pltpu.make_async_remote_copy(
            src_ref=src,
            dst_ref=dst,
            send_sem=send.at[PHASES.index(phase)],
            recv_sem=recv.at[PHASES.index(phase)],
            device_id=peer,
            device_id_type=MESH,
        ).start()

    def arrived(phase, ref):
        with jax.named_scope(f"wait_{phase}"):
            pltpu.make_async_copy(ref, ref, recv.at[PHASES.index(phase)]).wait()

    def left(phase, ref):
        pltpu.make_async_copy(ref, ref, send.at[PHASES.index(phase)]).wait()

    with jax.named_scope("load0"):
        for copy in loads[:2]:
            copy.wait()
    nodes = n_ref[...]
    r_q = iota((owners, owners), 1)
    k_of, dz_of = r_q // nz, r_q % nz
    q_of = (
        ((z + dz_of) & (nz - 1)) * nxc
        + ((x + (k_of >> 1)) & (nx - 1)) * 2
        + (c ^ (k_of & 1))
    )
    perm_q = hot(iota((owners, owners), 0) == q_of)
    sl_hot = hot(iota((nd, owners), 0) == sl_ref[...])
    sl_perm = dot(sl_hot, perm_q).astype(BF16)
    rows_out = t_dot(sl_perm, nodes).astype(BF16)
    for copy in loads[2:3]:
        copy.wait()
    p_out[...] = dot(rows_out, win_ref[1]).reshape(owners, 1, hs_w)
    p_in[0] = p_out[0]
    for k in range(nxc):
        out1[k] = rows_out[k * nz : (k + 1) * nz]
    r1[0] = rows_out[0:nz]

    early = (3, 4, 10, 12, 13)
    for i in early:
        loads[i].wait()
    gn = gn_ref[...]
    gn_w = dot_t(gn, wno_ref[...])
    base_n = dot(nodes, wn_ref[0]) + bn_ref[...]
    nb_b[0] = gn_w.astype(BF16)
    nb_b[1] = base_n.astype(BF16)

    with jax.named_scope("entry"):
        pl.semaphore_wait(barrier, len(peers))

    hw2, dw2, fw2 = hs_w // 2, d_feat // 2, fs_w // 2
    for d in far_first(ny):
        push("wout", wout_ref.at[pl.ds(c * hw2, hw2)], wout_g.at[d - 1, c], at_y(d))
    for d in far_first(ny):
        push("wn2", wn_ref.at[1, pl.ds(c * dw2, dw2)], wn2_g.at[d - 1, c], at_y(d))
    for d in far_first(ny):
        push("nb", nb_b, nb_g.at[d - 1], at_y(d))

    for k, d in everyone:
        push("halo", p_out.at[k * nz + d], p_in.at[k * nz + d], at_xc(k) | at_z(d))
    for k in range(1, nxc):
        push("raw1", out1.at[k], r1.at[k], at_xc(k))

    def hand_on(phase, buf):
        arrived(phase, buf.at[:, c])
        for d in far_first(ny):
            push(phase + "_c", buf.at[d - 1, c], buf.at[d - 1, c], {"c": 1 - c})

    for i in range(5, len(loads)):
        if i not in early:
            loads[i].wait()
    snd, rcv = snd_ref[...].reshape(1, ed), rcv_ref[...].reshape(1, ed)

    def remote(k, dz):
        owner_of = (
            ((z - dz) & (nz - 1)) * nxc
            + ((x - (k >> 1)) & (nx - 1)) * 2
            + (c ^ (k & 1))
        )
        return hot(owner_of + nd == snd)

    t_e = iota((owners, ed), 0)
    hot_pt = remote(t_e // nz, t_e % nz)
    hot_ht = remote(t_e % nxc, t_e // nxc)
    hot_st = hot(iota((nd, ed), 0) == snd)
    hot_rt = hot(iota((nd, ed), 0) == rcv)

    def picked(onehot, table):
        return dot(onehot, jnp.concatenate(two_parts(table), axis=0))

    def twice(onehot_t):
        return jnp.concatenate([jnp.transpose(onehot_t)] * 2, axis=1)

    hot_p[...] = twice(hot_pt)
    hot_r[...] = twice(hot_rt)

    live = jnp.concatenate(
        [
            jnp.where(iota((block, hs_w), 0) < vc_ref[b], 1.0, 0.0)
            for b in range(ed // block)
        ],
        axis=0,
    )
    edges = e_ref[...]
    base = (
        dot(edges, win_ref[0])
        + be_ref[...]
        + picked(twice(hot_st), dot(nodes, win_ref[1]))
        + picked(hot_r[...], dot(nodes, win_ref[2]))
    )
    ge = ge_ref[...]
    wout = wout_ref[...]
    ge_w = dot_t(ge, wout)

    n_t[...] = jnp.transpose(nodes)
    gn_t[...] = jnp.transpose(gn)
    e_t[...] = jnp.transpose(edges)

    t_i = iota((owners, owners), 0)
    stage = hot(iota((owners, owners), 1) == (t_i % nxc) * nz + t_i // nxc)
    arrived("raw1", r1.at[pl.ds(1, nxc - 1)])
    second = dot(stage, r1[...].reshape(owners, d_feat)).astype(BF16)
    for d in range(nz):
        out2[d] = second[d * nxc : (d + 1) * nxc]
    r2[0] = second[0:nxc]
    for d in far_first(nz):
        push("raw2", out2.at[d], r2.at[d], at_z(d))
    hand_on("wout", wout_g)

    arrived("halo", p_in.at[pl.ds(1, owners - 1)])
    pre = base + picked(hot_p[...], p_in[...].reshape(owners, hs_w))
    sg = sigmoid(pre)
    hidden = (pre * sg * live).astype(BF16)
    slope = sg * (1.0 + pre * (1.0 - sg)) * live
    hs = dot(hot_rt, hidden).astype(BF16)
    hs_b[...] = hs
    for d in far_first(ny):
        push("hs", hs_b, hs_g.at[d - 1], at_y(d))
    hand_on("wn2", wn2_g)
    geo = t_dot(ge, hidden)
    arrived("wout_c", wout_g.at[:, 1 - c])
    arrived("wn2_c", wn2_g.at[:, 1 - c])
    arrived("nb", nb_g)
    wout_f[0:hs_w] = wout
    wn2_f[:, 0:hs_w] = wn_ref[1]
    for d in range(1, ny):
        share = slice(d * hs_w, (d + 1) * hs_w)
        wout_f[share] = wout_g[d - 1].reshape(hs_w, d_feat)
        wn2_f[:, share] = wn2_g[d - 1].reshape(d_feat, hs_w)
    both[...] = dot(wout_f[...], wn2_f[...]).astype(BF16)
    before = jnp.concatenate(
        [base_n] + [nb_g[d - 1, 1].astype(F32) for d in range(1, ny)], axis=1
    )
    gradient = jnp.concatenate(
        [gn_w] + [nb_g[d - 1, 0].astype(F32) for d in range(1, ny)], axis=1
    )

    arrived("hs", hs_g)
    for d in far_first(ny):
        yd = pl.multiple_of(lax.rem(y + d, ny) * fs_w + c * fw2, fw2)
        push("rows", win_ref.at[:, pl.ds(yd, fw2)], rows_g.at[d - 1, c], at_y(d))
        push("wn1", wn_ref.at[0, pl.ds(yd, fw2)], wn1_g.at[d - 1, c], at_y(d))
    hs_f = jnp.concatenate([hs] + [hs_g[d - 1] for d in range(1, ny)], axis=1)
    npre = before + dot(hs_f, both[...])
    nsg = sigmoid(npre)
    nhid = (npre * nsg)[:, 0:hs_w].astype(BF16)
    npg_f = (gradient * (nsg * (1.0 + npre * (1.0 - nsg)))).astype(BF16)
    npgs = [npg_f[:, d * hs_w : (d + 1) * hs_w] for d in range(ny)]
    npg = npgs[0]
    agg = dot(hs_f, wout_f[...]).astype(BF16)

    ni, eo, ei = 2 * d_feat // owners, d_feat // owners, 3 * d_feat // owners

    def owner(n):
        return n % 2, (n // 2) % nx, n // nxc

    def in_fours(start, size, value):
        fours = value.reshape(-1, 4, hs_w).astype(BF16)
        for n in range(owners):
            oc, ox, oz = owner(n)
            for i in range(size // 4):
                ha[oc, ox, oz, start // 4 + i] = fours[n * size // 4 + i]

    in_fours(
        0, ni, jnp.concatenate([dot(n_t[...], npg), t_dot(agg, npg)], axis=0)
    )
    in_fours(ni, eo, dot(gn_t[...], nhid))
    push("core_a", ha.at[1 - c], ca, {"c": 1 - c})

    epg = ((ge_w + picked(hot_r[...], dot_t(npg_f, both[0:hs_w]))) * slope).astype(BF16)
    epg_b[...] = epg
    for d in far_first(ny):
        push("epg", epg_b, epg_g.at[d - 1], at_y(d))

    def add_core(phase, own, got, to, out, slots):
        arrived(phase, got)
        out[...] = (own[c].astype(F32) + got[...].astype(F32)).astype(BF16)
        for d in far_first(nx):
            xd = lax.rem(x + d, nx)
            push(to, out.at[xd], slots.at[d - 1], {"x": xd})

    def add_x(phase, own, got, to, out, slots):
        arrived(phase, got)
        total = own[x].astype(F32)
        for d in range(1, nx):
            total += got[d - 1].astype(F32)
        out[...] = total.astype(BF16)
        for d in far_first(nz):
            zd = lax.rem(z + d, nz)
            push(to, out.at[zd], slots.at[d - 1], {"z": zd})

    def add_z(phase, own, got):
        arrived(phase, got)
        total = own[z].astype(F32)
        for d in range(1, nz):
            total += got[d - 1].astype(F32)
        return total

    grad_agg = dot_t(npg_f, wn2_f[...]).astype(BF16)
    s_sum = dot(hot_st, epg)
    s_hot = s_sum.astype(BF16)
    h_hot = dot(hot_ht, epg).astype(BF16)
    r_hot = dot(hot_rt, epg).astype(BF16)
    g3[...] = geo + t_dot(grad_agg, hs)
    g1[0:d_feat] = dot(e_t[...], epg)
    g1[2 * d_feat :] = dot(n_t[...], r_hot)
    add_core("core_a", ha, ca, "x_a", xa, rxa)
    arrived("raw2", r2.at[pl.ds(1, nz - 1)])
    halo = r2[...].reshape(owners, d_feat)
    g1[d_feat : 2 * d_feat] = dot(n_t[...], s_hot) + t_dot(halo, h_hot)
    for n in range(owners):
        oc, ox, oz = owner(n)
        gb_f[oc, ox, oz, 0:ei] = g1[n * ei : (n + 1) * ei]
        gb_f[oc, ox, oz, ei:] = g3[n * eo : (n + 1) * eo]
    hb[...] = gb_f[...].astype(BF16)
    push("core_b", hb.at[1 - c], cb, {"c": 1 - c})

    back_out[...] = dot(hot_pt, epg).reshape(owners, 1, hs_w)
    back_in[0] = back_out[0]
    add_core("core_b", hb, cb, "x_b", xb, rxb)
    for k, d in everyone:
        at = k * nz + d
        push("back", back_out.at[at], back_in.at[at], at_xc(k, -1) | at_z(d, -1))
    hand_on("rows", rows_g)
    hand_on("wn1", wn1_g)
    add_x("x_a", xa, rxa, "z_a", za, rza)

    mine = pl.ds(pl.multiple_of(y * fs_w, fs_w), fs_w)
    arrived("epg", epg_g)
    arrived("rows_c", rows_g.at[:, 1 - c])
    arrived("wn1_c", wn1_g.at[:, 1 - c])
    w_s = [win_ref[1, mine]]
    grad_e = ge_ref[:, mine].astype(F32) + dot_t(epg, win_ref[0, mine])
    grad_n = (
        gn_ref[:, mine].astype(F32)
        + dot_t(npg, wn_ref[0, mine])
        + dot_t(r_hot, win_ref[2, mine])
    )
    for d in range(1, ny):
        part = epg_g[d - 1]
        r_d = dot(hot_rt, part).astype(BF16)
        w_e, w_sender, w_r = (
            jnp.concatenate([rows_g[d - 1, 0, b], rows_g[d - 1, 1, b]], axis=0)
            for b in range(3)
        )
        w_s.append(w_sender)
        grad_e += dot_t(part, w_e)
        grad_n += dot_t(r_d, w_r) + dot_t(npgs[d], wn1_g[d - 1].reshape(fs_w, hs_w))
    o_wide[0:ed] = grad_e.astype(BF16)

    add_x("x_b", xb, rxb, "z_b", zb, rzb)

    arrived("back", back_in.at[pl.ds(1, owners - 1)])
    high, low = two_parts(back_in[...].reshape(owners, hs_w))
    sums = (s_sum + dot(sl_perm, high) + dot(sl_perm, low)).astype(BF16)
    sums_b[...] = sums
    for d in far_first(ny):
        push("sums", sums_b, sums_g.at[d - 1], at_y(d))
    total_a = add_z("z_a", za, rza)
    for i in range(total_a.shape[0]):
        o_rows[4 * i : 4 * i + 4] = total_a[i]
    grad_n += dot_t(sums, w_s[0])
    arrived("sums", sums_g)
    for d in range(1, ny):
        grad_n += dot_t(sums_g[d - 1], w_s[d])
    o_wide[ed:] = grad_n.astype(BF16)
    left("halo", p_in.at[pl.ds(1, owners - 1)])
    left("raw1", out1.at[pl.ds(1, nxc - 1)])
    left("raw2", out2.at[pl.ds(1, nz - 1)])
    for phase, buf in (
        ("wout", wout_g),
        ("wn2", wn2_g),
        ("rows", rows_g),
        ("wn1", wn1_g),
    ):
        left(phase, buf.at[:, c])
        left(phase + "_c", buf.at[:, c])
    left("nb", nb_g)
    left("hs", hs_g)
    left("epg", epg_g)
    left("core_a", ca)
    left("core_b", cb)
    left("x_a", rxa)
    left("x_b", rxb)
    left("z_a", rza)
    left("z_b", rzb)
    left("back", back_in.at[pl.ds(1, owners - 1)])
    left("sums", sums_g)

    total_b = add_z("z_b", zb, rzb)
    o_rows[ni + eo :] = total_b


def hand_out(wide, rows, o_nodes, o_edges, o_ei, o_eo, o_ni, o_no):
    ed, ni, eo, ei = o_edges.shape[0], o_ni.shape[0], o_eo.shape[0], o_ei.shape[0]
    second = rows.shape[0] - ei - eo
    o_edges[...] = wide[0:ed]
    o_nodes[...] = wide[ed:]
    o_ni[...] = rows[0:ni]
    o_no[...] = rows[ni : ni + eo]
    o_ei[...] = rows[second : second + ei]
    o_eo[...] = rows[second + ei :]


def body(nz, nx, ny, nodes, edges, gn, ge, win, be, wout, wn, bn, wno, snd, rcv, vc, sl):
    nd, d = nodes.shape
    ed = edges.shape[0]
    hw = wout.shape[0]
    fw = d // ny
    nxc = 2 * nx
    owners = nz * nxc
    ni, eo, ei = 2 * d // owners, d // owners, 3 * d // owners
    ra = (ni + eo) // 4
    rb = ei + eo
    vm = pltpu.VMEM
    phases = len(PHASES)
    v_spec = pl.BlockSpec(memory_space=pltpu.VMEM)
    wide, rows = pl.pallas_call(
        functools.partial(kernel, nz, nx, ny),
        out_shape=(vm((ed + nd, fw), BF16), vm((4 * ra + rb, hw), F32)),
        in_specs=[pl.BlockSpec(memory_space=pl.ANY)] * 14,
        out_specs=(v_spec,) * 2,
        scratch_shapes=[
            vm((1, owners), jnp.int32),
            vm((ed,), jnp.int32),
            vm((ed,), jnp.int32),
            pltpu.SMEM((vc.shape[0],), jnp.int32),
            vm((nd, d), BF16),
            vm((ed, d), BF16),
            vm((nd, d), BF16),
            vm((ed, d), BF16),
            vm((3, d, hw), BF16),
            vm((1, hw), F32),
            vm((hw, d), BF16),
            vm((2, d, hw), BF16),
            vm((1, hw), F32),
            vm((hw, d), BF16),
            pltpu.SemaphoreType.DMA((14,)),
            vm((owners, 1, hw), F32),
            vm((owners, 1, hw), F32),
            vm((nxc, nz, d), BF16),
            vm((nxc, nz, d), BF16),
            vm((nz, nxc, d), BF16),
            vm((nz, nxc, d), BF16),
            vm((ny - 1, 2, hw // 2, d), BF16),
            vm((ny - 1, 2, d // 2, hw), BF16),
            vm((ny - 1, 2, 3, fw // 2, hw), BF16),
            vm((ny - 1, 2, fw // 2, hw), BF16),
            vm((2, nd, hw), BF16),
            vm((ny - 1, 2, nd, hw), BF16),
            vm((nd, hw), BF16),
            vm((ny - 1, nd, hw), BF16),
            vm((ed, hw), BF16),
            vm((ny - 1, ed, hw), BF16),
            vm((2, nx, nz, rb, hw), F32),
            vm((3 * d, hw), F32),
            vm((d, hw), F32),
            vm((2, nx, nz, ra, 4, hw), BF16),
            vm((2, nx, nz, rb, hw), BF16),
            vm((nx, nz, ra, 4, hw), BF16),
            vm((nx, nz, rb, hw), BF16),
            vm((nx, nz, ra, 4, hw), BF16),
            vm((nx, nz, rb, hw), BF16),
            vm((nx - 1, nz, ra, 4, hw), BF16),
            vm((nx - 1, nz, rb, hw), BF16),
            vm((nz, ra, 4, hw), BF16),
            vm((nz, rb, hw), BF16),
            vm((nz - 1, ra, 4, hw), BF16),
            vm((nz - 1, rb, hw), BF16),
            vm((owners, 1, hw), F32),
            vm((owners, 1, hw), F32),
            vm((nd, hw), BF16),
            vm((ny - 1, nd, hw), BF16),
            vm((ed, 2 * owners), BF16),
            vm((ed, 2 * nd), BF16),
            vm((d, nd), BF16),
            vm((d, nd), BF16),
            vm((d, ed), BF16),
            vm((ny * hw, d), BF16),
            vm((d, ny * hw), BF16),
            vm((ny * hw, ny * hw), BF16),
            pltpu.SemaphoreType.DMA((phases,)),
            pltpu.SemaphoreType.DMA((phases,)),
        ],
        compiler_params=pltpu.CompilerParams(collective_id=0, has_side_effects=True),
    )(
        sl.reshape(1, owners),
        snd,
        rcv,
        vc,
        nodes,
        edges,
        gn,
        ge,
        win.reshape(3, d, hw),
        be.reshape(1, hw),
        wout,
        wn.reshape(2, d, hw),
        bn.reshape(1, hw),
        wno,
    )
    g_nodes, g_edges, g_ei, g_eo, g_ni, g_no = pl.pallas_call(
        hand_out,
        out_shape=(
            jax.ShapeDtypeStruct((nd, fw), BF16),
            jax.ShapeDtypeStruct((ed, fw), BF16),
            jax.ShapeDtypeStruct((ei, hw), F32),
            jax.ShapeDtypeStruct((eo, hw), F32),
            jax.ShapeDtypeStruct((ni, hw), F32),
            jax.ShapeDtypeStruct((eo, hw), F32),
        ),
        in_specs=[v_spec] * 2,
        out_specs=(v_spec,) * 6,
    )(*(pltpu.with_memory_space_constraint(v, pltpu.VMEM) for v in (wide, rows)))
    return g_nodes, g_edges, g_ei, g_eo.T, g_ni, g_no.T


def solution(mesh):
    ny = mesh.shape["chan"]
    nx = 4 if mesh.shape["node"] == 128 else 2
    nz = mesh.shape["node"] // (2 * nx)
    split = Mesh(mesh.devices.reshape(nz, nx, 2, ny), ("z", "x", "c", "y"))
    in_specs = (
        P(NODE, None),
        P(NODE, None),
        P(NODE, None),
        P(NODE, None),
        P(None, "y"),
        P("y"),
        P("y", None),
        P(None, "y"),
        P("y"),
        P("y", None),
        P(NODE),
        P(NODE),
        P(NODE),
        P(NODE, None),
    )
    out_specs = (
        P(NODE, "y"),
        P(NODE, "y"),
        P(NODE, "y"),
        P("y", NODE),
        P(NODE, "y"),
        P("y", NODE),
    )
    return jax.shard_map(
        functools.partial(body, nz, nx, ny),
        mesh=split,
        in_specs=in_specs,
        out_specs=out_specs,
        check_vma=False,
    )
```

```python
import functools

import jax
import jax.numpy as jnp
from jax import lax
from jax.experimental import pallas as pl
from jax.experimental.pallas import tpu as pltpu
from jax.sharding import Mesh
from jax.sharding import PartitionSpec as P

NODE = ("z", "x", "c")
MESH = pl.DeviceIdType.MESH
F32 = jnp.float32
BF16 = jnp.bfloat16


def dot(a, b):
    return jnp.dot(a, b, preferred_element_type=F32)


def dot_t(a, b):
    return lax.dot_general(a, b, (((1,), (1,)), ((), ())), preferred_element_type=F32)


def t_dot(a, b):
    return lax.dot_general(a, b, (((0,), (0,)), ((), ())), preferred_element_type=F32)


def iota(shape, dim):
    return lax.broadcasted_iota(jnp.int32, shape, dim)


def hot(cond):
    return jnp.where(cond, 1.0, 0.0).astype(BF16)


def two_parts(v):
    high = v.astype(BF16)
    return high, (v - high.astype(F32)).astype(BF16)


def sigmoid(v):
    return 1.0 / (1.0 + jnp.exp(-v))


PHASES = (
    "halo",
    "raw1",
    "raw2",
    "wout",
    "wout_c",
    "wn2",
    "wn2_c",
    "nb",
    "rows",
    "rows_c",
    "wn1",
    "wn1_c",
    "hs",
    "epg",
    "core_a",
    "core_b",
    "x_a",
    "x_b",
    "z_a",
    "z_b",
    "back",
    "sums",
)


def kernel(
    nz,
    nx,
    ny,
    sl_in,
    snd_in,
    rcv_in,
    vc_in,
    n_in,
    e_in,
    gn_in,
    ge_in,
    win_in,
    be_in,
    wout_in,
    wn_in,
    bn_in,
    wno_in,
    o_wide,
    o_rows,
    sl_ref,
    snd_ref,
    rcv_ref,
    vc_ref,
    n_ref,
    e_ref,
    gn_ref,
    ge_ref,
    win_ref,
    be_ref,
    wout_ref,
    wn_ref,
    bn_ref,
    wno_ref,
    load,
    p_out,
    p_in,
    out1,
    r1,
    out2,
    r2,
    wout_g,
    wn2_g,
    rows_g,
    wn1_g,
    nb_b,
    nb_g,
    hs_b,
    hs_g,
    epg_b,
    epg_g,
    gb_f,
    g1,
    g3,
    ha,
    hb,
    ca,
    cb,
    xa,
    xb,
    rxa,
    rxb,
    za,
    zb,
    rza,
    rzb,
    back_out,
    back_in,
    sums_b,
    sums_g,
    hot_p,
    hot_r,
    n_t,
    gn_t,
    e_t,
    wout_f,
    wn2_f,
    both,
    send,
    recv,
):
    z, x, c, y = (lax.axis_index(a) for a in ("z", "x", "c", "y"))
    nxc = 2 * nx
    owners = nz * nxc
    nd, d_feat = n_ref.shape
    ed = e_ref.shape[0]
    hs_w = wout_ref.shape[0]
    fs_w = d_feat // ny
    block = ed // vc_ref.shape[0]

    def by(**kw):
        return kw

    def at_xc(k, sign=1):
        place = {}
        if k // 2:
            place["x"] = lax.rem(x + nx + sign * (k // 2), nx)
        if k % 2:
            place["c"] = 1 - c
        return place

    def at_z(d, sign=1):
        return {"z": lax.rem(z + nz + sign * d, nz)} if d else {}

    def at_y(d):
        return {"y": lax.rem(y + d, ny)}

    def hops(k, d):
        return min(d, nz - d) + min(k // 2, nx - k // 2)

    def far_first(n):
        return sorted(range(1, n), key=lambda d: -min(d, n - d))

    everyone = [(k, d) for k in range(nxc) for d in range(nz) if k or d]
    everyone.sort(key=lambda kd: -hops(*kd))

    sources = (sl_in, n_in, win_in, wout_in, wn_in, e_in, snd_in, rcv_in, vc_in, be_in, bn_in, ge_in, gn_in, wno_in)
    places = (sl_ref, n_ref, win_ref, wout_ref, wn_ref, e_ref, snd_ref, rcv_ref, vc_ref, be_ref, bn_ref, ge_ref, gn_ref, wno_ref)
    loads = [pltpu.make_async_copy(a, b, load.at[i]) for i, (a, b) in enumerate(zip(sources, places))]

    barrier = pltpu.get_barrier_semaphore()
    peers = [at_xc(k) | at_z(d) for k, d in everyone] + [at_y(d) for d in range(1, ny)]
    for peer in peers:
        pl.semaphore_signal(barrier, inc=1, device_id=peer, device_id_type=MESH)
    for copy in loads:
        copy.start()

    def push(phase, src, dst, peer):
        pltpu.make_async_remote_copy(
            src_ref=src,
            dst_ref=dst,
            send_sem=send.at[PHASES.index(phase)],
            recv_sem=recv.at[PHASES.index(phase)],
            device_id=peer,
            device_id_type=MESH,
        ).start()

    def arrived(phase, ref):
        with jax.named_scope(f"wait_{phase}"):
            pltpu.make_async_copy(ref, ref, recv.at[PHASES.index(phase)]).wait()

    def left(phase, ref):
        pltpu.make_async_copy(ref, ref, send.at[PHASES.index(phase)]).wait()

    with jax.named_scope("load0"):
        for copy in loads[:2]:
            copy.wait()
    nodes = n_ref[...]
    r_q = iota((owners, owners), 1)
    k_of, dz_of = r_q // nz, r_q % nz
    q_of = (
        ((z + dz_of) & (nz - 1)) * nxc
        + ((x + (k_of >> 1)) & (nx - 1)) * 2
        + (c ^ (k_of & 1))
    )
    perm_q = hot(iota((owners, owners), 0) == q_of)
    sl_hot = hot(iota((nd, owners), 0) == sl_ref[...])
    sl_perm = dot(sl_hot, perm_q).astype(BF16)
    rows_out = t_dot(sl_perm, nodes).astype(BF16)
    for copy in loads[2:3]:
        copy.wait()
    p_out[...] = dot(rows_out, win_ref[1]).reshape(owners, 1, hs_w)
    p_in[0] = p_out[0]
    for k in range(nxc):
        out1[k] = rows_out[k * nz : (k + 1) * nz]
    r1[0] = rows_out[0:nz]

    with jax.named_scope("entry"):
        pl.semaphore_wait(barrier, len(peers))

    for k, d in everyone:
        push("halo", p_out.at[k * nz + d], p_in.at[k * nz + d], at_xc(k) | at_z(d))
    for k in range(1, nxc):
        push("raw1", out1.at[k], r1.at[k], at_xc(k))

    hw2, dw2, fw2 = hs_w // 2, d_feat // 2, fs_w // 2
    for copy in loads[3:5]:
        copy.wait()
    for d in far_first(ny):
        push("wout", wout_ref.at[pl.ds(c * hw2, hw2)], wout_g.at[d - 1, c], at_y(d))
    for d in far_first(ny):
        push("wn2", wn_ref.at[1, pl.ds(c * dw2, dw2)], wn2_g.at[d - 1, c], at_y(d))

    def hand_on(phase, buf):
        arrived(phase, buf.at[:, c])
        for d in far_first(ny):
            push(phase + "_c", buf.at[d - 1, c], buf.at[d - 1, c], {"c": 1 - c})

    for copy in loads[5:]:
        copy.wait()
    gn = gn_ref[...]
    gn_w = dot_t(gn, wno_ref[...])
    base_n = dot(nodes, wn_ref[0]) + bn_ref[...]
    nb_b[0] = gn_w.astype(BF16)
    nb_b[1] = base_n.astype(BF16)
    for d in far_first(ny):
        push("nb", nb_b, nb_g.at[d - 1], at_y(d))

    snd, rcv = snd_ref[...].reshape(1, ed), rcv_ref[...].reshape(1, ed)

    def remote(k, dz):
        owner_of = (
            ((z - dz) & (nz - 1)) * nxc
            + ((x - (k >> 1)) & (nx - 1)) * 2
            + (c ^ (k & 1))
        )
        return hot(owner_of + nd == snd)

    t_e = iota((owners, ed), 0)
    hot_pt = remote(t_e // nz, t_e % nz)
    hot_ht = remote(t_e % nxc, t_e // nxc)
    hot_st = hot(iota((nd, ed), 0) == snd)
    hot_rt = hot(iota((nd, ed), 0) == rcv)

    def picked(onehot, table):
        return dot(onehot, jnp.concatenate(two_parts(table), axis=0))

    def twice(onehot_t):
        return jnp.concatenate([jnp.transpose(onehot_t)] * 2, axis=1)

    hot_p[...] = twice(hot_pt)
    hot_r[...] = twice(hot_rt)

    live = jnp.concatenate(
        [
            jnp.where(iota((block, hs_w), 0) < vc_ref[b], 1.0, 0.0)
            for b in range(ed // block)
        ],
        axis=0,
    )
    edges = e_ref[...]
    base = (
        dot(edges, win_ref[0])
        + be_ref[...]
        + picked(twice(hot_st), dot(nodes, win_ref[1]))
        + picked(hot_r[...], dot(nodes, win_ref[2]))
    )
    ge = ge_ref[...]
    wout = wout_ref[...]
    ge_w = dot_t(ge, wout)

    n_t[...] = jnp.transpose(nodes)
    gn_t[...] = jnp.transpose(gn)
    e_t[...] = jnp.transpose(edges)

    t_i = iota((owners, owners), 0)
    stage = hot(iota((owners, owners), 1) == (t_i % nxc) * nz + t_i // nxc)
    arrived("raw1", r1.at[pl.ds(1, nxc - 1)])
    second = dot(stage, r1[...].reshape(owners, d_feat)).astype(BF16)
    for d in range(nz):
        out2[d] = second[d * nxc : (d + 1) * nxc]
    r2[0] = second[0:nxc]
    for d in far_first(nz):
        push("raw2", out2.at[d], r2.at[d], at_z(d))
    hand_on("wout", wout_g)

    arrived("halo", p_in.at[pl.ds(1, owners - 1)])
    pre = base + picked(hot_p[...], p_in[...].reshape(owners, hs_w))
    sg = sigmoid(pre)
    hidden = (pre * sg * live).astype(BF16)
    slope = sg * (1.0 + pre * (1.0 - sg)) * live
    hs = dot(hot_rt, hidden).astype(BF16)
    hs_b[...] = hs
    for d in far_first(ny):
        push("hs", hs_b, hs_g.at[d - 1], at_y(d))
    hand_on("wn2", wn2_g)
    geo = t_dot(ge, hidden)
    arrived("wout_c", wout_g.at[:, 1 - c])
    arrived("wn2_c", wn2_g.at[:, 1 - c])
    arrived("nb", nb_g)
    wout_f[0:hs_w] = wout
    wn2_f[:, 0:hs_w] = wn_ref[1]
    for d in range(1, ny):
        share = slice(d * hs_w, (d + 1) * hs_w)
        wout_f[share] = wout_g[d - 1].reshape(hs_w, d_feat)
        wn2_f[:, share] = wn2_g[d - 1].reshape(d_feat, hs_w)
    both[...] = dot(wout_f[...], wn2_f[...]).astype(BF16)
    before = jnp.concatenate(
        [base_n] + [nb_g[d - 1, 1].astype(F32) for d in range(1, ny)], axis=1
    )
    gradient = jnp.concatenate(
        [gn_w] + [nb_g[d - 1, 0].astype(F32) for d in range(1, ny)], axis=1
    )

    arrived("hs", hs_g)
    for d in far_first(ny):
        yd = pl.multiple_of(lax.rem(y + d, ny) * fs_w + c * fw2, fw2)
        push("rows", win_ref.at[:, pl.ds(yd, fw2)], rows_g.at[d - 1, c], at_y(d))
        push("wn1", wn_ref.at[0, pl.ds(yd, fw2)], wn1_g.at[d - 1, c], at_y(d))
    hs_f = jnp.concatenate([hs] + [hs_g[d - 1] for d in range(1, ny)], axis=1)
    npre = before + dot(hs_f, both[...])
    nsg = sigmoid(npre)
    nhid = (npre * nsg)[:, 0:hs_w].astype(BF16)
    npg_f = (gradient * (nsg * (1.0 + npre * (1.0 - nsg)))).astype(BF16)
    npgs = [npg_f[:, d * hs_w : (d + 1) * hs_w] for d in range(ny)]
    npg = npgs[0]
    agg = dot(hs_f, wout_f[...]).astype(BF16)

    ni, eo, ei = 2 * d_feat // owners, d_feat // owners, 3 * d_feat // owners

    def owner(n):
        return n % 2, (n // 2) % nx, n // nxc

    def in_fours(start, size, value):
        fours = value.reshape(-1, 4, hs_w).astype(BF16)
        for n in range(owners):
            oc, ox, oz = owner(n)
            for i in range(size // 4):
                ha[oc, ox, oz, start // 4 + i] = fours[n * size // 4 + i]

    in_fours(
        0, ni, jnp.concatenate([dot(n_t[...], npg), t_dot(agg, npg)], axis=0)
    )
    in_fours(ni, eo, dot(gn_t[...], nhid))
    push("core_a", ha.at[1 - c], ca, {"c": 1 - c})

    epg = ((ge_w + picked(hot_r[...], dot_t(npg_f, both[0:hs_w]))) * slope).astype(BF16)
    epg_b[...] = epg
    for d in far_first(ny):
        push("epg", epg_b, epg_g.at[d - 1], at_y(d))

    def add_core(phase, own, got, to, out, slots):
        arrived(phase, got)
        out[...] = (own[c].astype(F32) + got[...].astype(F32)).astype(BF16)
        for d in far_first(nx):
            xd = lax.rem(x + d, nx)
            push(to, out.at[xd], slots.at[d - 1], {"x": xd})

    def add_x(phase, own, got, to, out, slots):
        arrived(phase, got)
        total = own[x].astype(F32)
        for d in range(1, nx):
            total += got[d - 1].astype(F32)
        out[...] = total.astype(BF16)
        for d in far_first(nz):
            zd = lax.rem(z + d, nz)
            push(to, out.at[zd], slots.at[d - 1], {"z": zd})

    def add_z(phase, own, got):
        arrived(phase, got)
        total = own[z].astype(F32)
        for d in range(1, nz):
            total += got[d - 1].astype(F32)
        return total

    grad_agg = dot_t(npg_f, wn2_f[...]).astype(BF16)
    s_sum = dot(hot_st, epg)
    s_hot = s_sum.astype(BF16)
    h_hot = dot(hot_ht, epg).astype(BF16)
    r_hot = dot(hot_rt, epg).astype(BF16)
    g3[...] = geo + t_dot(grad_agg, hs)
    g1[0:d_feat] = dot(e_t[...], epg)
    g1[2 * d_feat :] = dot(n_t[...], r_hot)
    arrived("raw2", r2.at[pl.ds(1, nz - 1)])
    halo = r2[...].reshape(owners, d_feat)
    g1[d_feat : 2 * d_feat] = dot(n_t[...], s_hot) + t_dot(halo, h_hot)
    for n in range(owners):
        oc, ox, oz = owner(n)
        gb_f[oc, ox, oz, 0:ei] = g1[n * ei : (n + 1) * ei]
        gb_f[oc, ox, oz, ei:] = g3[n * eo : (n + 1) * eo]
    hb[...] = gb_f[...].astype(BF16)
    push("core_b", hb.at[1 - c], cb, {"c": 1 - c})
    add_core("core_a", ha, ca, "x_a", xa, rxa)

    back_out[...] = dot(hot_pt, epg).reshape(owners, 1, hs_w)
    back_in[0] = back_out[0]
    add_core("core_b", hb, cb, "x_b", xb, rxb)
    for k, d in everyone:
        at = k * nz + d
        push("back", back_out.at[at], back_in.at[at], at_xc(k, -1) | at_z(d, -1))
    hand_on("rows", rows_g)
    hand_on("wn1", wn1_g)
    add_x("x_a", xa, rxa, "z_a", za, rza)

    mine = pl.ds(pl.multiple_of(y * fs_w, fs_w), fs_w)
    arrived("epg", epg_g)
    arrived("rows_c", rows_g.at[:, 1 - c])
    arrived("wn1_c", wn1_g.at[:, 1 - c])
    w_s = [win_ref[1, mine]]
    grad_e = ge_ref[:, mine].astype(F32) + dot_t(epg, win_ref[0, mine])
    grad_n = (
        gn_ref[:, mine].astype(F32)
        + dot_t(npg, wn_ref[0, mine])
        + dot_t(r_hot, win_ref[2, mine])
    )
    for d in range(1, ny):
        part = epg_g[d - 1]
        r_d = dot(hot_rt, part).astype(BF16)
        w_e, w_sender, w_r = (
            jnp.concatenate([rows_g[d - 1, 0, b], rows_g[d - 1, 1, b]], axis=0)
            for b in range(3)
        )
        w_s.append(w_sender)
        grad_e += dot_t(part, w_e)
        grad_n += dot_t(r_d, w_r) + dot_t(npgs[d], wn1_g[d - 1].reshape(fs_w, hs_w))
    o_wide[0:ed] = grad_e.astype(BF16)

    add_x("x_b", xb, rxb, "z_b", zb, rzb)

    arrived("back", back_in.at[pl.ds(1, owners - 1)])
    high, low = two_parts(back_in[...].reshape(owners, hs_w))
    sums = (s_sum + dot(sl_perm, high) + dot(sl_perm, low)).astype(BF16)
    sums_b[...] = sums
    for d in far_first(ny):
        push("sums", sums_b, sums_g.at[d - 1], at_y(d))
    total_a = add_z("z_a", za, rza)
    for i in range(total_a.shape[0]):
        o_rows[4 * i : 4 * i + 4] = total_a[i]
    grad_n += dot_t(sums, w_s[0])
    arrived("sums", sums_g)
    for d in range(1, ny):
        grad_n += dot_t(sums_g[d - 1], w_s[d])
    o_wide[ed:] = grad_n.astype(BF16)
    left("halo", p_in.at[pl.ds(1, owners - 1)])
    left("raw1", out1.at[pl.ds(1, nxc - 1)])
    left("raw2", out2.at[pl.ds(1, nz - 1)])
    for phase, buf in (
        ("wout", wout_g),
        ("wn2", wn2_g),
        ("rows", rows_g),
        ("wn1", wn1_g),
    ):
        left(phase, buf.at[:, c])
        left(phase + "_c", buf.at[:, c])
    left("nb", nb_g)
    left("hs", hs_g)
    left("epg", epg_g)
    left("core_a", ca)
    left("core_b", cb)
    left("x_a", rxa)
    left("x_b", rxb)
    left("z_a", rza)
    left("z_b", rzb)
    left("back", back_in.at[pl.ds(1, owners - 1)])
    left("sums", sums_g)

    total_b = add_z("z_b", zb, rzb)
    o_rows[ni + eo :] = total_b


def hand_out(wide, rows, o_nodes, o_edges, o_ei, o_eo, o_ni, o_no):
    ed, ni, eo, ei = o_edges.shape[0], o_ni.shape[0], o_eo.shape[0], o_ei.shape[0]
    second = rows.shape[0] - ei - eo
    o_edges[...] = wide[0:ed]
    o_nodes[...] = wide[ed:]
    o_ni[...] = rows[0:ni]
    o_no[...] = rows[ni : ni + eo]
    o_ei[...] = rows[second : second + ei]
    o_eo[...] = rows[second + ei :]


def body(nz, nx, ny, nodes, edges, gn, ge, win, be, wout, wn, bn, wno, snd, rcv, vc, sl):
    nd, d = nodes.shape
    ed = edges.shape[0]
    hw = wout.shape[0]
    fw = d // ny
    nxc = 2 * nx
    owners = nz * nxc
    ni, eo, ei = 2 * d // owners, d // owners, 3 * d // owners
    ra = (ni + eo) // 4
    rb = ei + eo
    vm = pltpu.VMEM
    phases = len(PHASES)
    v_spec = pl.BlockSpec(memory_space=pltpu.VMEM)
    wide, rows = pl.pallas_call(
        functools.partial(kernel, nz, nx, ny),
        out_shape=(vm((ed + nd, fw), BF16), vm((4 * ra + rb, hw), F32)),
        in_specs=[pl.BlockSpec(memory_space=pl.ANY)] * 14,
        out_specs=(v_spec,) * 2,
        scratch_shapes=[
            vm((1, owners), jnp.int32),
            vm((ed,), jnp.int32),
            vm((ed,), jnp.int32),
            pltpu.SMEM((vc.shape[0],), jnp.int32),
            vm((nd, d), BF16),
            vm((ed, d), BF16),
            vm((nd, d), BF16),
            vm((ed, d), BF16),
            vm((3, d, hw), BF16),
            vm((1, hw), F32),
            vm((hw, d), BF16),
            vm((2, d, hw), BF16),
            vm((1, hw), F32),
            vm((hw, d), BF16),
            pltpu.SemaphoreType.DMA((14,)),
            vm((owners, 1, hw), F32),
            vm((owners, 1, hw), F32),
            vm((nxc, nz, d), BF16),
            vm((nxc, nz, d), BF16),
            vm((nz, nxc, d), BF16),
            vm((nz, nxc, d), BF16),
            vm((ny - 1, 2, hw // 2, d), BF16),
            vm((ny - 1, 2, d // 2, hw), BF16),
            vm((ny - 1, 2, 3, fw // 2, hw), BF16),
            vm((ny - 1, 2, fw // 2, hw), BF16),
            vm((2, nd, hw), BF16),
            vm((ny - 1, 2, nd, hw), BF16),
            vm((nd, hw), BF16),
            vm((ny - 1, nd, hw), BF16),
            vm((ed, hw), BF16),
            vm((ny - 1, ed, hw), BF16),
            vm((2, nx, nz, rb, hw), F32),
            vm((3 * d, hw), F32),
            vm((d, hw), F32),
            vm((2, nx, nz, ra, 4, hw), BF16),
            vm((2, nx, nz, rb, hw), BF16),
            vm((nx, nz, ra, 4, hw), BF16),
            vm((nx, nz, rb, hw), BF16),
            vm((nx, nz, ra, 4, hw), BF16),
            vm((nx, nz, rb, hw), BF16),
            vm((nx - 1, nz, ra, 4, hw), BF16),
            vm((nx - 1, nz, rb, hw), BF16),
            vm((nz, ra, 4, hw), BF16),
            vm((nz, rb, hw), BF16),
            vm((nz - 1, ra, 4, hw), BF16),
            vm((nz - 1, rb, hw), BF16),
            vm((owners, 1, hw), F32),
            vm((owners, 1, hw), F32),
            vm((nd, hw), BF16),
            vm((ny - 1, nd, hw), BF16),
            vm((ed, 2 * owners), BF16),
            vm((ed, 2 * nd), BF16),
            vm((d, nd), BF16),
            vm((d, nd), BF16),
            vm((d, ed), BF16),
            vm((ny * hw, d), BF16),
            vm((d, ny * hw), BF16),
            vm((ny * hw, ny * hw), BF16),
            pltpu.SemaphoreType.DMA((phases,)),
            pltpu.SemaphoreType.DMA((phases,)),
        ],
        compiler_params=pltpu.CompilerParams(collective_id=0, has_side_effects=True),
    )(
        sl.reshape(1, owners),
        snd,
        rcv,
        vc,
        nodes,
        edges,
        gn,
        ge,
        win.reshape(3, d, hw),
        be.reshape(1, hw),
        wout,
        wn.reshape(2, d, hw),
        bn.reshape(1, hw),
        wno,
    )
    g_nodes, g_edges, g_ei, g_eo, g_ni, g_no = pl.pallas_call(
        hand_out,
        out_shape=(
            jax.ShapeDtypeStruct((nd, fw), BF16),
            jax.ShapeDtypeStruct((ed, fw), BF16),
            jax.ShapeDtypeStruct((ei, hw), F32),
            jax.ShapeDtypeStruct((eo, hw), F32),
            jax.ShapeDtypeStruct((ni, hw), F32),
            jax.ShapeDtypeStruct((eo, hw), F32),
        ),
        in_specs=[v_spec] * 2,
        out_specs=(v_spec,) * 6,
    )(*(pltpu.with_memory_space_constraint(v, pltpu.VMEM) for v in (wide, rows)))
    return g_nodes, g_edges, g_ei, g_eo.T, g_ni, g_no.T


def solution(mesh):
    ny = mesh.shape["chan"]
    nx = 4 if mesh.shape["node"] == 128 else 2
    nz = mesh.shape["node"] // (2 * nx)
    split = Mesh(mesh.devices.reshape(nz, nx, 2, ny), ("z", "x", "c", "y"))
    in_specs = (
        P(NODE, None),
        P(NODE, None),
        P(NODE, None),
        P(NODE, None),
        P(None, "y"),
        P("y"),
        P("y", None),
        P(None, "y"),
        P("y"),
        P("y", None),
        P(NODE),
        P(NODE),
        P(NODE),
        P(NODE, None),
    )
    out_specs = (
        P(NODE, "y"),
        P(NODE, "y"),
        P(NODE, "y"),
        P("y", NODE),
        P(NODE, "y"),
        P("y", NODE),
    )
    return jax.shard_map(
        functools.partial(body, nz, nx, ny),
        mesh=split,
        in_specs=in_specs,
        out_specs=out_specs,
        check_vma=False,
    )
```
